16 devices in a mesh: dp: 2 (over y, z), cp: 8 (over x, core).
Axes of the slice: x: 4, y: 2, z: 1, core: 2. Of those that a mesh axis runs over, the one named last changes fastest.
The devices are a block of a 4x4x8 slice.
Arguments:
- queries: bfloat16 [768, 32, 128], P(('dp', 'cp')), parts along dimension 0
- key_new: bfloat16 [768, 8, 128], P(('dp', 'cp')), parts along dimension 0
- value_new: bfloat16 [768, 8, 128], P(('dp', 'cp')), parts along dimension 0
- key_cache: bfloat16 [24576, 8, 128], P(('dp', 'cp')), parts along dimension 0
- value_cache: bfloat16 [24576, 8, 128], P(('dp', 'cp')), parts along dimension 0
- prefix_len: int32 [2], P('dp'), parts along dimension 0
Outputs:
- output 1: bfloat16 [768, 32, 128], P(('dp', 'cp')), parts along dimension 0
- output 2: float32 [768, 32], P(('dp', 'cp')), parts along dimension 0
There are 2 independent parts. The reference program is written for one: setup_inputs(seed, part) draws one part's arguments, and reference() takes and returns one part's arrays. A program takes and returns all parts, laid end to end along the dimension named above; each array names one.
All inputs are finite; a program needn't handle non-finite values.
Results may differ from the reference program's by a relative error of at most 0.00895518.
Values are sent between devices in bfloat16 or wider.
A program may use at most 768 MiB of HBM per device.

```python
import math
import jax
import jax.numpy as jnp
from jax import lax

GROUP_SIZE = 8
NEW_DEV = 48
PREFIX_DEV = 1536
Q_HEADS = 32
KV_HEADS = 8
HEAD_DIM = 128
NEW_LEN = GROUP_SIZE * NEW_DEV
P_MAX = GROUP_SIZE * PREFIX_DEV
GROUP_RATIO = Q_HEADS // KV_HEADS


def setup_inputs(seed: int = 0, part: int = 0) -> dict:
    base_key = jax.random.fold_in(jax.random.key(seed), part)
    rand_keys = jax.random.split(base_key, 9)
    shift_scale = GROUP_SIZE ** 0.5
    new_boost = math.log(P_MAX / NEW_LEN) * 2.0 ** 0.5
    direction = jax.random.normal(rand_keys[0], (KV_HEADS, HEAD_DIM), jnp.float32)
    direction = direction / jnp.linalg.norm(direction, axis=-1, keepdims=True)
    q_mean = jnp.repeat(direction, GROUP_RATIO, axis=0) * HEAD_DIM ** 0.5
    q_noise = jax.random.normal(rand_keys[1], (NEW_LEN, Q_HEADS, HEAD_DIM), jnp.float32)
    queries = (q_noise + q_mean[None]) * 0.5 ** 0.5
    key_new = jax.random.normal(rand_keys[2], (NEW_LEN, KV_HEADS, HEAD_DIM), jnp.float32) + new_boost * direction[None]
    new_shift = jax.random.normal(rand_keys[3], (GROUP_SIZE, 1, KV_HEADS, HEAD_DIM), jnp.float32) * shift_scale
    value_new = jax.random.normal(rand_keys[4], (GROUP_SIZE, NEW_DEV, KV_HEADS, HEAD_DIM), jnp.float32) + new_shift
    key_cache = jax.random.normal(rand_keys[5], (P_MAX, KV_HEADS, HEAD_DIM), jnp.float32)
    cache_shift = jax.random.normal(rand_keys[6], (GROUP_SIZE, 1, KV_HEADS, HEAD_DIM), jnp.float32) * shift_scale
    value_cache = jax.random.normal(rand_keys[7], (GROUP_SIZE, PREFIX_DEV, KV_HEADS, HEAD_DIM), jnp.float32) + cache_shift
    prefix_len = jax.random.randint(rand_keys[8], (1,), (3 * P_MAX) // 4, P_MAX + 1, jnp.int32)
    return {
        'queries': queries.astype(jnp.bfloat16),
        'key_new': key_new.astype(jnp.bfloat16),
        'value_new': value_new.reshape(NEW_LEN, KV_HEADS, HEAD_DIM).astype(jnp.bfloat16),
        'key_cache': key_cache.astype(jnp.bfloat16),
        'value_cache': value_cache.reshape(P_MAX, KV_HEADS, HEAD_DIM).astype(jnp.bfloat16),
        'prefix_len': prefix_len,
    }


def reference(queries, key_new, value_new, key_cache, value_cache, prefix_len):
    prefix_end = prefix_len[0]
    key_pos = jnp.arange(P_MAX + NEW_LEN)
    logit_scale = HEAD_DIM ** -0.5

    def one_head(head_idx):
        kv_idx = head_idx // GROUP_RATIO
        keys_all = jnp.concatenate([lax.dynamic_index_in_dim(key_cache, kv_idx, axis=1, keepdims=False), lax.dynamic_index_in_dim(key_new, kv_idx, axis=1, keepdims=False)], axis=0).astype(jnp.float32)
        vals_all = jnp.concatenate([lax.dynamic_index_in_dim(value_cache, kv_idx, axis=1, keepdims=False), lax.dynamic_index_in_dim(value_new, kv_idx, axis=1, keepdims=False)], axis=0).astype(jnp.float32)
        q_head = lax.dynamic_index_in_dim(queries, head_idx, axis=1, keepdims=False).astype(jnp.float32).reshape(GROUP_SIZE, NEW_DEV, HEAD_DIM)

        def one_block(block_args):
            q_rows, row_start = block_args
            scores = jnp.dot(q_rows, keys_all.T) * logit_scale
            q_pos = row_start + jnp.arange(NEW_DEV)
            visible = jnp.where(key_pos[None, :] < P_MAX, key_pos[None, :] < prefix_end, key_pos[None, :] - P_MAX <= q_pos[:, None])
            scores = jnp.where(visible, scores, -jnp.inf)
            row_max = jnp.max(scores, axis=-1)
            exp_scores = jnp.exp(scores - row_max[:, None])
            row_sum = jnp.sum(exp_scores, axis=-1)
            prob_bf = exp_scores.astype(jnp.bfloat16).astype(jnp.float32)
            block_out = jnp.dot(prob_bf, vals_all) / row_sum[:, None]
            return block_out.astype(jnp.bfloat16), row_max + jnp.log(row_sum)

        head_out, head_lse = lax.map(one_block, (q_head, jnp.arange(GROUP_SIZE) * NEW_DEV))
        return head_out.reshape(NEW_LEN, HEAD_DIM), head_lse.reshape(NEW_LEN)

    all_out, all_lse = lax.map(one_head, jnp.arange(Q_HEADS))
    return jnp.transpose(all_out, (1, 0, 2)), jnp.transpose(all_lse)
```

```python
import functools
import math

import jax
import jax.numpy as jnp
from jax import lax
from jax.experimental import pallas as pl
from jax.experimental.pallas import tpu as pltpu
from jax.sharding import PartitionSpec as P

MESH = pl.DeviceIdType.MESH
NEG = -1e30
CH = 256
BF = jnp.bfloat16
F32 = jnp.float32


def attend_kernel(n, scale, plen, q, kc, vt, kn, vn, o_out, l_out,
                  kb, vb, vnb, qb, ob, lb, osend, lsend, s0, s1, mscr,
                  kvl, kvs, kvr, qls, qss, qrs, fss, oss, ors, lss, lrs):
    S = (s0, s1)
    heads, rows, dim = q.shape[1], q.shape[2], q.shape[3]
    cl, nl = kc.shape[2], kn.shape[2]
    cols = 2 * rows
    grp = rows // nl
    c2 = float(scale * math.log2(math.e))
    nch = n // 2
    me = lax.axis_index('cp')
    x, h = me // 2, lax.rem(me, 2)
    oh = 1 - h
    xl, xr, xd = lax.rem(x + nch - 1, nch), lax.rem(x + 1, nch), lax.rem(x + 2, nch)
    src_chip = (x, xl, xr, xd)

    def dev(chip, core):
        return {'cp': chip * 2 + core}

    def remote(src, dst, ss, rs, chip, core):
        return pltpu.make_async_remote_copy(src_ref=src, dst_ref=dst, send_sem=ss, recv_sem=rs,
                                            device_id=dev(chip, core), device_id_type=MESH)

    bar = pltpu.get_barrier_semaphore()
    for j in range(1, n):
        pl.semaphore_signal(bar, inc=1, device_id={'cp': lax.rem(me + j, n)}, device_id_type=MESH)

    def kv_parts(k, half, core):
        return ((kc.at[half, k], kb.at[k, pl.ds(pl.multiple_of(core * cl, 128), cl)]),
                (vt.at[half, k], vb.at[k, :, pl.ds(pl.multiple_of(core * cl, 128), cl)]),
                (kn.at[half, k], kb.at[k, pl.ds(pl.multiple_of(2 * cl + core * nl, 16), nl)]),
                (vn.at[half, k], vnb.at[k, pl.ds(pl.multiple_of(core * nl, 16), nl)]))

    def kv_local(k):
        return [pltpu.make_async_copy(s, d, kvl.at[k, i]) for i, (s, d) in enumerate(kv_parts(k, h, h))]

    def kv_remote(k):
        return [remote(s, d, kvs.at[k, i], kvr.at[k, i], x, oh) for i, (s, d) in enumerate(kv_parts(k, oh, h))]

    def q_local(k):
        return pltpu.make_async_copy(q.at[h, k], qb.at[0, k, pl.ds(pl.multiple_of(h * rows, 16), rows)], qls.at[k])

    def q_remote(k):
        out = []
        dst = pl.ds(pl.multiple_of(h * rows, 16), rows)
        i = 0
        for chip, rel in ((xl, 2), (xr, 1)):
            for core in (0, 1):
                out.append(remote(q.at[core, k], qb.at[rel, k, dst], qss.at[i, k], qrs.at[rel, h, k], chip, core))
                i += 1
        out.append(remote(q.at[oh, k], qb.at[0, k, dst], qss.at[i, k], qrs.at[0, h, k], x, oh))
        return out

    def q_arrive(rel, core, k):
        d = qb.at[rel, k, pl.ds(pl.multiple_of(core * rows, 16), rows)]
        return pltpu.make_async_copy(d, d, qrs.at[rel, core, k])

    def forward(k, way):
        rel, chip = ((1, xr), (2, xl))[way]
        piece = pl.ds(way * rows, rows)
        return remote(qb.at[rel, k, piece], qb.at[3, k, piece], fss.at[way, k], qrs.at[3, way, k], chip, h)

    for k in range(heads):
        for cp in kv_local(k):
            cp.start()
        q_local(k).start()
    pl.semaphore_wait(bar, n - 1)
    for k in range(heads):
        for cp in q_remote(k):
            cp.start()
        for cp in kv_remote(k):
            cp.start()

    def wait_kv(k):
        for cp in kv_local(k):
            cp.wait()
        for i, (s, d) in enumerate(kv_parts(k, h, oh)):
            pltpu.make_async_copy(d, d, kvr.at[k, i]).wait()

    def wait_q(k, c):
        if c == 0:
            q_local(k).wait()
            q_arrive(0, oh, k).wait()
        else:
            q_arrive(c, 0, k).wait()
            q_arrive(c, 1, k).wait()

    nkeys = 2 * cl + 2 * nl
    bounds = [(a, min(a + CH, 2 * cl)) for a in range(0, 2 * cl, CH)] + [(2 * cl, nkeys)]
    pref = plen[0] - x * (2 * cl)

    def score_chunk(k, qv, c, a, e, dst, mx):
        s = lax.dot_general(kb[k, a:e, :], qv, (((1,), (1,)), ((), ())), preferred_element_type=F32)
        if a < 2 * cl:
            seen = (lax.broadcasted_iota(jnp.int32, (e - a, 1), 0) + a) < pref
            s = jnp.where(seen, s, NEG)
        else:
            key = lax.broadcasted_iota(jnp.int32, (e - a, cols), 0) + x * (2 * nl)
            tok = lax.broadcasted_iota(jnp.int32, (e - a, cols), 1) // grp + src_chip[c] * (2 * nl)
            s = jnp.where(key <= tok, s, NEG)
        dst[a:e, :] = s
        mb = jnp.max(s.reshape((e - a) // 8, 8, cols), axis=0)
        return mb if mx is None else jnp.maximum(mx, mb)

    def value_chunk(k, a, e, srcs, mc, o, l):
        s = srcs[a:e, :]
        p = jnp.exp2(s * c2 - mc)
        lsum = jnp.sum(p.reshape((e - a) // 8, 8, cols), axis=0)
        vv = vb[k, :, a:e] if a < 2 * cl else vnb[k].T
        oo = jnp.dot(vv, p.astype(BF), preferred_element_type=F32)
        return (oo if o is None else o + oo), (lsum if l is None else l + lsum)

    def close_scores(slot, mx):
        mscr[slot] = jnp.broadcast_to(jnp.max(mx, axis=0, keepdims=True) * c2, (8, cols))

    def close_values(k, c, slot, o, l):
        u = k * 4 + c
        ls = jnp.sum(l, axis=0, keepdims=True)
        on = (o * (1.0 / ls)).T.astype(BF)
        osend[u] = on
        lsend[u] = mscr[slot][0:1, :] + jnp.log2(ls)

    def o_copies(k, c, a, core_static=None):
        u = k * 4 + c
        rel = (0, 2, 1, 3)[c]
        hh = h * heads + k
        return (remote(osend.at[u, pl.ds(pl.multiple_of(a * rows, 16), rows)], ob.at[rel, hh], oss.at[u, a], ors.at[rel, hh],
                       src_chip[c], a),
                remote(lsend.at[u], lb.at[rel, hh], lss.at[u, a], lrs.at[rel, hh], src_chip[c], a))

    def send_unit(k, c):
        if c == 0:
            for cp in o_copies(k, 0, oh):
                cp.start()
        else:
            for a in (0, 1):
                for cp in o_copies(k, c, a):
                    cp.start()

    def step(k, c, nxt):
        slot = c % 2
        mc = mscr[slot][0:1, :]
        mx = o = l = None
        if nxt is not None:
            k2, cc2 = nxt
            qv = qb[cc2, k2]
        for a, e in bounds:
            if nxt is not None:
                mx = score_chunk(k2, qv, cc2, a, e, S[1 - slot], mx)
            o, l = value_chunk(k, a, e, S[slot], mc, o, l)
        if nxt is not None:
            close_scores(1 - slot, mx)
        close_values(k, c, slot, o, l)

    def forwards(k):
        for way, rel in ((0, 1), (1, 2)):
            q_arrive(rel, way, k).wait()
            forward(k, way).start()

    def wait_q_rest(k, c):
        if c in (1, 2):
            q_arrive(c, 2 - c, k).wait()
        else:
            wait_q(k, c)

    wait_kv(0)
    wait_q(0, 0)
    mx = None
    q00 = qb[0, 0]
    for a, e in bounds:
        mx = score_chunk(0, q00, 0, a, e, s0, mx)
    close_scores(0, mx)
    forwards(0)

    def head_body(k, last):
        for c in range(4):
            if c < 3:
                wait_q_rest(k, c + 1)
                nxt = (k, c + 1)
            elif not last:
                wait_kv(k + 1)
                wait_q(k + 1, 0)
                nxt = (k + 1, 0)
            else:
                nxt = None
            if c == 2 and not last:
                forwards(k + 1)
            step(k, c, nxt)
            send_unit(k, c)

    def loop_body(k, carry):
        head_body(k, False)
        return carry

    lax.fori_loop(0, heads - 1, loop_body, 0)
    head_body(heads - 1, True)

    my = pl.ds(pl.multiple_of(h * rows, 16), rows)

    def own_l(hd_core, u):
        return None

    for hc in (0, 1):
        def comb(k, carry):
            hh = hc * heads + k

            @pl.when(hc != h)
            def _():
                d = ob.at[0, hh]
                pltpu.make_async_copy(d, d, ors.at[0, hh]).wait()
                d = lb.at[0, hh]
                pltpu.make_async_copy(d, d, lrs.at[0, hh]).wait()

            @pl.when(hc == h)
            def _():
                ob[0, hh] = osend[k * 4, my, :]
                lb[0, hh] = lsend[k * 4]

            for rel in (1, 2, 3):
                d = ob.at[rel, hh]
                pltpu.make_async_copy(d, d, ors.at[rel, hh]).wait()
                d = lb.at[rel, hh]
                pltpu.make_async_copy(d, d, lrs.at[rel, hh]).wait()
            ls = [lb[r, hh] for r in range(4)]
            ls = [jnp.where(h == 0, v[:, :rows], v[:, rows:]) for v in ls]
            m = jnp.maximum(jnp.maximum(ls[0], ls[1]), jnp.maximum(ls[2], ls[3]))
            w = [jnp.exp2(v - m) for v in ls]
            tot = (w[0] + w[1]) + (w[2] + w[3])
            inv = 1.0 / tot
            wt = jnp.concatenate([v * inv for v in w] + [jnp.zeros((4, rows), F32)], axis=0).T
            acc = None
            for r in range(4):
                t = ob[r, hh].astype(F32) * wt[:, r:r + 1]
                acc = t if acc is None else acc + t
            o_out[hh] = acc.astype(BF)
            l_out[hh] = (m + jnp.log2(tot)) * float(math.log(2.0))
            return carry
        lax.fori_loop(0, heads, comb, 0)

    def drain(k, carry):
        for cp in q_remote(k):
            cp.wait_send()
        for cp in kv_remote(k):
            cp.wait_send()
        for way in (0, 1):
            forward(k, way).wait_send()
        for c in range(4):
            if c == 0:
                for cp in o_copies(k, 0, oh):
                    cp.wait_send()
            else:
                for a in (0, 1):
                    for cp in o_copies(k, c, a):
                        cp.wait_send()
        return carry
    lax.fori_loop(0, heads, drain, 0)


def solution(mesh):
    n = mesh.shape['cp']
    tok = P(('dp', 'cp'))

    def local(queries, key_new, value_new, key_cache, value_cache, prefix_len):
        t, qh, d = queries.shape
        cl, kh = key_cache.shape[0], key_cache.shape[1]
        g = qh // kh
        hv = kh // 2
        rows = t * g
        nkeys = 2 * cl + 2 * t
        q = queries.reshape(t, kh, g, d).transpose(1, 0, 2, 3).reshape(2, hv, rows, d)
        kc = key_cache.transpose(1, 0, 2).reshape(2, hv, cl, d)
        vt = value_cache.transpose(1, 2, 0).reshape(2, hv, d, cl)
        kn = key_new.transpose(1, 0, 2).reshape(2, hv, t, d)
        vn = value_new.transpose(1, 0, 2).reshape(2, hv, t, d)
        anyspec = pl.BlockSpec(memory_space=pl.ANY)
        vm = pl.BlockSpec(memory_space=pltpu.VMEM)
        dma = pltpu.SemaphoreType.DMA
        o, l = pl.pallas_call(
            functools.partial(attend_kernel, n, d ** -0.5),
            name='attend',
            out_shape=(jax.ShapeDtypeStruct((kh, rows, d), BF), jax.ShapeDtypeStruct((kh, 1, rows), F32)),
            in_specs=[pl.BlockSpec(memory_space=pltpu.SMEM)] + [anyspec] * 5,
            out_specs=(vm, vm),
            scratch_shapes=[
                pltpu.VMEM((hv, nkeys, d), BF),
                pltpu.VMEM((hv, d, 2 * cl), BF),
                pltpu.VMEM((hv, 2 * t, d), BF),
                pltpu.VMEM((4, hv, 2 * rows, d), BF),
                pltpu.VMEM((4, kh, rows, d), BF),
                pltpu.VMEM((4, kh, 1, 2 * rows), F32),
                pltpu.VMEM((4 * hv, 2 * rows, d), BF),
                pltpu.VMEM((4 * hv, 1, 2 * rows), F32),
                pltpu.VMEM((nkeys, 2 * rows), F32),
                pltpu.VMEM((nkeys, 2 * rows), F32),
                pltpu.VMEM((2, 8, 2 * rows), F32),
                dma((hv, 4)), dma((hv, 4)), dma((hv, 4)),
                dma((hv,)), dma((5, hv)), dma((4, 2, hv)), dma((2, hv)),
                dma((4 * hv, 2)), dma((4, kh)), dma((4 * hv, 2)), dma((4, kh)),
            ],
            compiler_params=pltpu.CompilerParams(collective_id=0, has_side_effects=True,
                                                 vmem_limit_bytes=60 * 2 ** 20),
        )(prefix_len, q, kc, vt, kn, vn)
        attn = o.reshape(kh, t, g, d).transpose(1, 0, 2, 3).reshape(t, qh, d)
        lse = l.reshape(kh, t, g).transpose(1, 0, 2).reshape(t, qh)
        return attn, lse

    return jax.shard_map(local, mesh=mesh, in_specs=(tok, tok, tok, tok, tok, P('dp')), out_specs=(tok, tok), check_vma=False)
```

```python
import functools
import math

import jax
import jax.numpy as jnp
from jax import lax
from jax.experimental import pallas as pl
from jax.experimental.pallas import tpu as pltpu
from jax.sharding import PartitionSpec as P

MESH = pl.DeviceIdType.MESH
NEG = -1e30
CH = 256
PREP = 256
PARTS = 3
BF = jnp.bfloat16
F32 = jnp.float32
LEFT, RIGHT, FAR = 1, 2, 3
UNITS = ((0, LEFT), (0, RIGHT), (1, LEFT), (1, RIGHT), (0, FAR), (1, FAR),
         (2, LEFT), (2, RIGHT), (2, FAR), (3, FAR), (3, LEFT), (3, RIGHT))


def pick(i, table):
    out = table[0]
    for j, v in enumerate(table[1:], 1):
        out = jnp.where(i == j, v, out)
    return out


def attend_kernel(n, scale, plen, q, kn, vn, kc, vc, o_out, l_out,
                  kb, vb, kst, vst, knst, vnst, prep, qb, ob, lb, osend, lsend, orel, lrel, s0, s1, mscr, lfin,
                  kvl, kvs, kvr, nvl, nvs, nvr, qss, qrs, fss, oss, ors, lss, lrs, rss, rrs, rls, rlr):
    S = (s0, s1)
    toks, heads, grp, dim = q.shape[0], q.shape[2], q.shape[3], q.shape[4]
    rows = toks * grp
    cols = 2 * rows
    cl = kc.shape[0]
    c2 = float(scale * math.log2(math.e))
    nch = n // 2
    me = lax.axis_index('cp')
    x, h = me // 2, lax.rem(me, 2)
    oh = 1 - h
    xl, xr, xd = lax.rem(x + nch - 1, nch), lax.rem(x + 1, nch), lax.rem(x + 2, nch)
    chips = (x, xl, xr, xd)

    def chip_of(c):
        return chips[c] if isinstance(c, int) else pick(c, chips)

    def remote(src, dst, ss, rs, chip, core):
        return pltpu.make_async_remote_copy(src_ref=src, dst_ref=dst, send_sem=ss, recv_sem=rs,
                                            device_id={'cp': chip * 2 + core}, device_id_type=MESH)

    def arrived(dst, sem):
        pltpu.make_async_copy(dst, dst, sem).wait()

    bar = pltpu.get_barrier_semaphore()
    for j in range(1, n):
        pl.semaphore_signal(bar, inc=1, device_id={'cp': lax.rem(me + j, n)}, device_id_type=MESH)

    part = cl // PARTS

    def kv_local(p):
        src = pl.ds(p * part, part)
        return [pltpu.make_async_copy(a.at[src, h], st.at[src], kvl.at[i, p]) for i, (a, st) in enumerate(((kc, kst), (vc, vst)))]

    def kv_remote(p):
        src, dst = pl.ds(p * part, part), pl.ds(cl + p * part, part)
        return [remote(a.at[src, oh], st.at[dst], kvs.at[i, p], kvr.at[i, p], x, oh) for i, (a, st) in enumerate(((kc, kst), (vc, vst)))]

    def kv_arrived(p):
        dst = pl.ds(cl + p * part, part)
        for i, st in enumerate((kst, vst)):
            arrived(st.at[dst], kvr.at[i, p])

    nrow = pl.ds(h * toks, toks)

    def new_local():
        return [pltpu.make_async_copy(a.at[:, h], st.at[nrow], nvl.at[i]) for i, (a, st) in enumerate(((kn, knst), (vn, vnst)))]

    def new_remote():
        return [remote(a.at[:, oh], st.at[nrow], nvs.at[i], nvr.at[i], x, oh) for i, (a, st) in enumerate(((kn, knst), (vn, vnst)))]

    def q_local(k):
        return pltpu.make_async_copy(q.at[:, h, k], qb.at[0, k, nrow], qrs.at[0, h, k])

    def q_partner(k):
        return remote(q.at[:, oh, k], qb.at[0, k, nrow], qss.at[4, k], qrs.at[0, h, k], x, oh)

    def q_remote(k):
        out = []
        for chip, rel in ((xl, RIGHT), (xr, LEFT)):
            for core in (0, 1):
                out.append(remote(q.at[:, core, k], qb.at[rel, k, nrow], qss.at[len(out), k], qrs.at[rel, h, k], chip, core))
        return out

    def q_arrived(rel, core, k):
        arrived(qb.at[rel, k, pl.ds(core * toks, toks)], qrs.at[rel, core, k])

    def forward(k, way):
        rel, chip = ((LEFT, xr), (RIGHT, xl))[way]
        piece = pl.ds(way * toks, toks)
        return remote(qb.at[rel, k, piece], qb.at[FAR, k, piece], fss.at[way, k], qrs.at[FAR, way, k], chip, h)

    def forwards(k):
        for way, rel in ((0, LEFT), (1, RIGHT)):
            q_arrived(rel, way, k)
            forward(k, way).start()

    for p in range(PARTS):
        for cp in kv_local(p):
            cp.start()
    for cp in new_local():
        cp.start()
    for k in range(heads):
        q_local(k).start()
    pl.semaphore_wait(bar, n - 1)
    for k in range(heads):
        q_partner(k).start()
    for cp in new_remote():
        cp.start()
    for k in range(heads):
        for cp in q_remote(k):
            cp.start()
    for p in range(PARTS):
        for cp in kv_remote(p):
            cp.start()

    def split(kraw, vraw, count, base):
        prep[0, 0:count * heads] = kraw.reshape(count * heads, dim).astype(F32)
        prep[1, 0:count * heads] = vraw.reshape(count * heads, dim).astype(F32)
        for j in range(heads):
            kb[j, pl.ds(base, count), :] = prep[0, pl.ds(j, count, stride=heads), :].astype(BF)
            vb[j, :, pl.ds(base, count)] = prep[1, pl.ds(j, count, stride=heads), :].astype(BF).T

    def split_part(first):
        def go(i, carry):
            base = pl.multiple_of(first + i * PREP, PREP)
            split(kst[pl.ds(base, PREP)], vst[pl.ds(base, PREP)], PREP, base)
            return carry
        lax.fori_loop(0, part // PREP, go, 0)

    pref = plen[0] - x * (2 * cl)
    own_b = [(a, a + CH) for a in range(0, cl, CH)]
    oth_b = [(a, a + CH) for a in range(cl, 2 * cl, CH)]
    new_b = [(2 * cl, 2 * cl + 2 * toks)]
    all_b = own_b + oth_b + new_b

    def score_chunk(k, qv, chip, a, e, dst, mx):
        s = lax.dot_general(kb[k, a:e, :], qv, (((1,), (1,)), ((), ())), preferred_element_type=F32)
        if a < 2 * cl:
            first = h * cl + a if a < cl else oh * cl + (a - cl)
            s = jnp.where(lax.broadcasted_iota(jnp.int32, (e - a, 1), 0) < pref - first, s, NEG)
        else:
            key = lax.broadcasted_iota(jnp.int32, (e - a, cols), 0)
            tok = lax.broadcasted_iota(jnp.int32, (e - a, cols), 1) // grp
            s = jnp.where(key - tok <= (chip - x) * (2 * toks), s, NEG)
        dst[a:e, :] = s
        mb = jnp.max(s.reshape((e - a) // 8, 8, cols), axis=0)
        return mb if mx is None else jnp.maximum(mx, mb)

    def value_chunk(k, a, e, src, mc, o, l):
        p = jnp.exp2(src[a:e, :] * c2 - mc)
        lsum = jnp.sum(p.reshape((e - a) // 8, 8, cols), axis=0)
        oo = jnp.dot(vb[k, :, a:e], p.astype(BF), preferred_element_type=F32)
        return (oo if o is None else o + oo), (lsum if l is None else l + lsum)

    def step(slot, cur, nxt):
        mx = o = l = None
        if nxt is not None:
            k2, r2, b2 = nxt
            qv = qb[r2, k2].reshape(cols, dim)
            chip = chip_of(r2)
        if cur is not None:
            k, b1, u = cur
            mc = mscr[slot][0:1, :]
        for i in range(max(len(b2) if nxt is not None else 0, len(b1) if cur is not None else 0)):
            if nxt is not None and i < len(b2):
                mx = score_chunk(k2, qv, chip, *b2[i], S[1 - slot], mx)
            if cur is not None and i < len(b1):
                o, l = value_chunk(k, *b1[i], S[slot], mc, o, l)
        if nxt is not None:
            mscr[1 - slot] = jnp.broadcast_to(jnp.max(mx, axis=0, keepdims=True) * c2, (8, cols))
        if cur is not None:
            ls = jnp.sum(l, axis=0, keepdims=True)
            osend[u] = (o * (1.0 / ls)).T.astype(BF)
            lse = mc + jnp.log2(ls)
            lsend[u, 0] = lse[:, :rows]
            lsend[u, 1] = lse[:, rows:]

    def slot_of(k, c):
        return k * 3 + (c - 1)

    def own_slot(k, half):
        return heads * 3 + half * heads + k

    def piece(a):
        return pl.ds(pl.multiple_of(a * rows, 16), rows)

    def result(u, a, dst_o, dst_l, so, sl, chip, core):
        return (remote(osend.at[u, piece(a)], dst_o, oss.at[u, a], so, chip, core),
                remote(lsend.at[u, a], dst_l, lss.at[u, a], sl, chip, core))

    hh_of = lambda k: h * heads + k

    def own_copies(k, half):
        hh = hh_of(k)
        rel = 3 * half
        return result(own_slot(k, half), oh, ob.at[rel, hh], lb.at[rel, hh], ors.at[rel, hh], lrs.at[rel, hh], x, oh)

    def side_copies(k, c):
        hh = hh_of(k)
        if isinstance(c, int):
            a, rel, chip = (c - 1), 3 - c, chips[c]
        else:
            a, rel, chip = c - 1, 3 - c, pick(c, chips)
        return result(slot_of(k, c), a, ob.at[rel, hh], lb.at[rel, hh], ors.at[rel, hh], lrs.at[rel, hh], chip, a)

    def far_copies(k, a):
        chip = (xr, xl)[a]
        return result(slot_of(k, FAR), a, orel.at[a, k], lrel.at[a, k], rrs.at[a, k], rlr.at[a, k], chip, h)

    def merged_copies(k, a):
        hh = hh_of(k)
        chip, rel = ((xr, LEFT), (xl, RIGHT))[a]
        return (remote(orel.at[a, heads + k], ob.at[rel, hh], rss.at[a, k], ors.at[rel, hh], chip, a),
                remote(lrel.at[a, heads + k], lb.at[rel, hh], rls.at[a, k], lrs.at[rel, hh], chip, a))

    def columns(ws):
        pad = jnp.zeros((8 - len(ws), rows), F32)
        return jnp.concatenate(list(ws) + [pad], axis=0).T

    def relay(k):
        for a in (0, 1):
            arrived(orel.at[a, k], rrs.at[a, k])
            arrived(lrel.at[a, k], rlr.at[a, k])
        for a in (0, 1):
            u = slot_of(k, (RIGHT, LEFT)[a])
            l0, l1 = lsend[u, a], lrel[a, k]
            m = jnp.maximum(l0, l1)
            w0, w1 = jnp.exp2(l0 - m), jnp.exp2(l1 - m)
            tot = w0 + w1
            inv = 1.0 / tot
            wt = columns((w0 * inv, w1 * inv))
            orel[a, heads + k] = (osend[u, a * rows:(a + 1) * rows, :].astype(F32) * wt[:, 0:1]
                                  + orel[a, k].astype(F32) * wt[:, 1:2]).astype(BF)
            lrel[a, heads + k] = m + jnp.log2(tot)
        for a in (0, 1):
            for cp in merged_copies(k, a):
                cp.start()

    def start(cps):
        for cp in cps:
            cp.start()

    def wait_q(k, c):
        if isinstance(c, int):
            if c != LEFT:
                q_arrived(c, 0, k)
            if c != RIGHT:
                q_arrived(c, 1, k)
        else:
            @pl.when(c != LEFT)
            def _():
                q_arrived(c, 0, k)

            @pl.when(c != RIGHT)
            def _():
                q_arrived(c, 1, k)

    def send_unit(k, c):
        if isinstance(c, int):
            if c == FAR:
                start(far_copies(k, 0))
                start(far_copies(k, 1))
            else:
                start(side_copies(k, c))
        else:
            @pl.when(c == FAR)
            def _():
                start(far_copies(k, 0))
                start(far_copies(k, 1))

            @pl.when(c != FAR)
            def _():
                start(side_copies(k, c))

    for p in range(PARTS):
        for cp in kv_local(p):
            cp.wait()
        split_part(p * part)
    wait_q(0, 0)
    step(1, None, (0, 0, own_b))
    for k in range(heads):
        if k + 1 < heads:
            wait_q(k + 1, 0)
        step(k % 2, (k, own_b, own_slot(k, 0)), (k + 1, 0, own_b) if k + 1 < heads else None)
        start(own_copies(k, 0))
        if k == 1:
            forwards(0)
    forwards(1)

    for cp in new_local():
        cp.wait()
    for i, st in enumerate((knst, vnst)):
        arrived(st.at[pl.ds(oh * toks, toks)], nvr.at[i])
    split(knst[...], vnst[...], 2 * toks, 2 * cl)
    for p in range(PARTS):
        kv_arrived(p)
        split_part(cl + p * part)
    forwards(2)

    def go(u, k, c, k2, c2_, slot):
        wait_q(k2, c2_)
        step(slot, (k, all_b, slot_of(k, c)), (k2, c2_, all_b))
        send_unit(k, c)

    hs, cs = [u[0] for u in UNITS], [u[1] for u in UNITS]
    wait_q(*UNITS[0])
    step(1, None, UNITS[0] + (all_b,))

    def pair(i, carry):
        u = 2 * i
        go(u, pick(u, hs), pick(u, cs), pick(u + 1, hs), pick(u + 1, cs), 0)

        @pl.when(i == 0)
        def _():
            forwards(3)
        go(u + 1, pick(u + 1, hs), pick(u + 1, cs), pick(u + 2, hs), pick(u + 2, cs), 1)

        @pl.when(i == 3)
        def _():
            relay(0)
            relay(1)
        return carry

    lax.fori_loop(0, len(UNITS) // 2 - 1, pair, 0)
    k, c = UNITS[-2]
    k2, c2_ = UNITS[-1]
    wait_q(k2, c2_)
    step(0, (k, all_b, slot_of(k, c)), (k2, c2_, all_b))
    send_unit(k, c)
    relay(2)
    rest = oth_b + new_b
    step(1, (k2, all_b, slot_of(k2, c2_)), (0, 0, rest))
    send_unit(k2, c2_)
    relay(3)

    for k in range(heads):
        step(k % 2, (k, rest, own_slot(k, 1)), (k + 1, 0, rest) if k + 1 < heads else None)
        start(own_copies(k, 1))

    def final(k, own):
        hh = (h if own else oh) * heads + k
        if own:
            parts = [(osend[own_slot(k, half), piece(h), :], lsend[own_slot(k, half), h]) for half in (0, 1)]
        else:
            for rel in (0, 3):
                arrived(ob.at[rel, hh], ors.at[rel, hh])
                arrived(lb.at[rel, hh], lrs.at[rel, hh])
            parts = [(ob[rel, hh], lb[rel, hh]) for rel in (0, 3)]
        parts += [(ob[rel, hh], lb[rel, hh]) for rel in (LEFT, RIGHT)]
        ls = [p[1] for p in parts]
        m = jnp.maximum(jnp.maximum(ls[0], ls[1]), jnp.maximum(ls[2], ls[3]))
        w = [jnp.exp2(v - m) for v in ls]
        tot = (w[0] + w[1]) + (w[2] + w[3])
        inv = 1.0 / tot
        wt = columns([v * inv for v in w])
        acc = None
        for r in range(4):
            t = parts[r][0].astype(F32) * wt[:, r:r + 1]
            acc = t if acc is None else acc + t
        o_out[:, hh] = acc.astype(BF).reshape(toks, grp, dim)
        lfin[pl.ds(hh, 1), :] = (m + jnp.log2(tot)) * float(math.log(2.0))

    for k in range(heads):
        for own in (True, False):
            hh = (h if own else oh) * heads + k
            for rel in (LEFT, RIGHT):
                arrived(ob.at[rel, hh], ors.at[rel, hh])
                arrived(lb.at[rel, hh], lrs.at[rel, hh])
        for own in (True, False):
            final(k, own)
    l_out[...] = lfin[...]

    def drain(k, carry):
        cps = list(q_remote(k)) + [q_partner(k), forward(k, 0), forward(k, 1)]
        for half in (0, 1):
            cps += own_copies(k, half)
        for c in (LEFT, RIGHT):
            cps += side_copies(k, c)
        for a in (0, 1):
            cps += far_copies(k, a)
            cps += merged_copies(k, a)
        for cp in cps:
            cp.wait_send()
        return carry
    lax.fori_loop(0, heads, drain, 0)
    for cp in new_remote():
        cp.wait_send()
    for p in range(PARTS):
        for cp in kv_remote(p):
            cp.wait_send()


def solution(mesh):
    n = mesh.shape['cp']
    tok = P(('dp', 'cp'))

    def local(queries, key_new, value_new, key_cache, value_cache, prefix_len):
        t, qh, d = queries.shape
        cl, kh = key_cache.shape[0], key_cache.shape[1]
        g = qh // kh
        hv = kh // 2
        rows = t * g
        nkeys = 2 * cl + 2 * t
        width = -(-nkeys // 128) * 128
        q = queries.reshape(t, 2, hv, g, d)
        kc, vc = (a.reshape(cl, 2, hv, d) for a in (key_cache, value_cache))
        kn, vn = (a.reshape(t, 2, hv, d) for a in (key_new, value_new))
        anyspec = pl.BlockSpec(memory_space=pl.ANY)
        vm = pl.BlockSpec(memory_space=pltpu.VMEM)
        dma = pltpu.SemaphoreType.DMA
        nres = 5 * hv
        o, l = pl.pallas_call(
            functools.partial(attend_kernel, n, d ** -0.5),
            name='attend',
            out_shape=(jax.ShapeDtypeStruct((t, kh, g, d), BF), jax.ShapeDtypeStruct((kh, rows), F32)),
            in_specs=[pl.BlockSpec(memory_space=pltpu.SMEM)] + [anyspec] * 5,
            out_specs=(vm, vm),
            scratch_shapes=[
                pltpu.VMEM((hv, nkeys, d), BF),
                pltpu.VMEM((hv, d, width), BF),
                pltpu.VMEM((2 * cl, hv, d), BF),
                pltpu.VMEM((2 * cl, hv, d), BF),
                pltpu.VMEM((2 * t, hv, d), BF),
                pltpu.VMEM((2 * t, hv, d), BF),
                pltpu.VMEM((2, PREP * hv, d), F32),
                pltpu.VMEM((4, hv, 2 * t, g, d), BF),
                pltpu.VMEM((4, kh, rows, d), BF),
                pltpu.VMEM((4, kh, 1, rows), F32),
                pltpu.VMEM((nres, 2 * rows, d), BF),
                pltpu.VMEM((nres, 2, 1, rows), F32),
                pltpu.VMEM((2, 2 * hv, rows, d), BF),
                pltpu.VMEM((2, 2 * hv, 1, rows), F32),
                pltpu.VMEM((nkeys, 2 * rows), F32),
                pltpu.VMEM((nkeys, 2 * rows), F32),
                pltpu.VMEM((2, 8, 2 * rows), F32),
                pltpu.VMEM((kh, rows), F32),
                dma((2, PARTS)), dma((2, PARTS)), dma((2, PARTS)),
                dma((2,)), dma((2,)), dma((2,)),
                dma((5, hv)), dma((4, 2, hv)), dma((2, hv)),
                dma((nres, 2)), dma((4, kh)), dma((nres, 2)), dma((4, kh)),
                dma((2, hv)), dma((2, hv)), dma((2, hv)), dma((2, hv)),
            ],
            compiler_params=pltpu.CompilerParams(collective_id=0, has_side_effects=True,
                                                 vmem_limit_bytes=62 * 2 ** 20),
        )(prefix_len, q, kn, vn, kc, vc)
        lse = l.reshape(kh, t, g).transpose(1, 0, 2).reshape(t, qh)
        return o.reshape(t, qh, d), lse

    return jax.shard_map(local, mesh=mesh, in_specs=(tok, tok, tok, tok, tok, P('dp')), out_specs=(tok, tok), check_vma=False)
```

```python
import functools
import math

import jax
import jax.numpy as jnp
from jax import lax
from jax.experimental import pallas as pl
from jax.experimental.pallas import tpu as pltpu
from jax.sharding import PartitionSpec as P

MESH = pl.DeviceIdType.MESH
NEG = -1e30
CH = 256
PREP = 256
PARTS = 3
LOOPED = 8
BF = jnp.bfloat16
F32 = jnp.float32
LEFT, RIGHT, FAR = 1, 2, 3
UNITS = ((0, LEFT), (0, RIGHT), (1, LEFT), (1, RIGHT), (0, FAR), (1, FAR),
         (2, LEFT), (2, RIGHT), (2, FAR), (3, FAR), (3, LEFT), (3, RIGHT))


def pick(i, table):
    out = table[0]
    for j, v in enumerate(table[1:], 1):
        out = jnp.where(i == j, v, out)
    return out


def attend_kernel(n, scale, plen, q, kn, vn, kc, vc, o_out, l_out,
                  kb, vb, kst, vst, knst, vnst, prep, qb, ob, lb, osend, lsend, orel, lrel, s0, s1, mscr, lfin, ltr,
                  kvl, kvs, kvr, nvl, nvs, nvr, qss, qrs, oss, ors, lss, lrs, rss, rrs, rls, rlr):
    S = (s0, s1)
    toks, heads, grp, dim = q.shape[0], q.shape[2], q.shape[3], q.shape[4]
    rows = toks * grp
    cols = 2 * rows
    cl = kc.shape[0]
    c2 = float(scale * math.log2(math.e))
    nch = n // 2
    me = lax.axis_index('cp')
    x, h = me // 2, lax.rem(me, 2)
    oh = 1 - h
    xl, xr, xd = lax.rem(x + nch - 1, nch), lax.rem(x + 1, nch), lax.rem(x + 2, nch)
    chips = (x, xl, xr, xd)

    def chip_of(c):
        return chips[c] if isinstance(c, int) else pick(c, chips)

    def remote(src, dst, ss, rs, chip, core):
        return pltpu.make_async_remote_copy(src_ref=src, dst_ref=dst, send_sem=ss, recv_sem=rs,
                                            device_id={'cp': chip * 2 + core}, device_id_type=MESH)

    def arrived(dst, sem):
        pltpu.make_async_copy(dst, dst, sem).wait()

    bar = pltpu.get_barrier_semaphore()
    for j in range(1, n):
        pl.semaphore_signal(bar, inc=1, device_id={'cp': lax.rem(me + j, n)}, device_id_type=MESH)

    part = cl // PARTS

    def kv_local(p):
        src = pl.ds(p * part, part)
        return [pltpu.make_async_copy(a.at[src, h], st.at[src], kvl.at[i, p]) for i, (a, st) in enumerate(((kc, kst), (vc, vst)))]

    def kv_remote(p):
        src, dst = pl.ds(p * part, part), pl.ds(cl + p * part, part)
        return [remote(a.at[src, oh], st.at[dst], kvs.at[i], kvr.at[i, p], x, oh) for i, (a, st) in enumerate(((kc, kst), (vc, vst)))]

    def kv_arrived(p):
        dst = pl.ds(cl + p * part, part)
        for i, st in enumerate((kst, vst)):
            arrived(st.at[dst], kvr.at[i, p])

    nrow = pl.ds(h * toks, toks)

    def new_local():
        return [pltpu.make_async_copy(a.at[:, h], st.at[nrow], nvl.at[i]) for i, (a, st) in enumerate(((kn, knst), (vn, vnst)))]

    def new_remote():
        return [remote(a.at[:, oh], st.at[nrow], nvs.at[i], nvr.at[i], x, oh) for i, (a, st) in enumerate(((kn, knst), (vn, vnst)))]

    def q_local(k):
        return pltpu.make_async_copy(q.at[:, h, k], qb.at[k, nrow], qrs.at[0, h, k])

    def q_partner(k):
        return remote(q.at[:, oh, k], qb.at[k, nrow], qss, qrs.at[0, h, k], x, oh)

    def q_remote(k):
        out = []
        for chip, rel in ((xl, RIGHT), (xr, LEFT)):
            for core in (0, 1):
                out.append(remote(q.at[:, core, k], qb.at[rel * heads + k, nrow], qss, qrs.at[rel, h, k], chip, core))
        return out

    def q_arrived(rel, core, k):
        arrived(qb.at[rel * heads + k, pl.ds(core * toks, toks)], qrs.at[rel, core, k])

    def forward(k, way):
        rel, chip = ((LEFT, xr), (RIGHT, xl))[way]
        piece = pl.ds(way * toks, toks)
        return remote(qb.at[rel * heads + k, piece], qb.at[FAR * heads + k, piece], qss, qrs.at[FAR, way, k], chip, h)

    def forwards(k):
        for way, rel in ((0, LEFT), (1, RIGHT)):
            q_arrived(rel, way, k)
            forward(k, way).start()

    for p in range(PARTS):
        for cp in kv_local(p):
            cp.start()
    for cp in new_local():
        cp.start()
    for k in range(heads):
        q_local(k).start()
    pl.semaphore_wait(bar, n - 1)
    for k in range(heads):
        q_partner(k).start()
    for cp in new_remote():
        cp.start()
    for k in range(heads):
        for cp in q_remote(k):
            cp.start()
    for p in range(PARTS):
        for cp in kv_remote(p):
            cp.start()

    def split(kraw, vraw, count, base):
        prep[0, 0:count * heads] = kraw.reshape(count * heads, dim).astype(F32)
        prep[1, 0:count * heads] = vraw.reshape(count * heads, dim).astype(F32)
        for j in range(heads):
            kb[j, pl.ds(base, count), :] = prep[0, pl.ds(j, count, stride=heads), :].astype(BF)
            vb[j, :, pl.ds(base, count)] = prep[1, pl.ds(j, count, stride=heads), :].astype(BF).T

    def split_part(first):
        def go(i, carry):
            base = pl.multiple_of(first + i * PREP, PREP)
            split(kst[pl.ds(base, PREP)], vst[pl.ds(base, PREP)], PREP, base)
            return carry
        lax.fori_loop(0, part // PREP, go, 0)

    pref = plen[0] - x * (2 * cl)
    own_b = [(a, a + CH) for a in range(0, cl, CH)]
    oth_b = [(a, a + CH) for a in range(cl, 2 * cl, CH)]
    new_b = [(2 * cl, 2 * cl + 2 * toks)]
    all_b = own_b + oth_b + new_b

    def score_chunk(k, qv, chip, a, e, dst, mx):
        s = lax.dot_general(kb[k, a:e, :], qv, (((1,), (1,)), ((), ())), preferred_element_type=F32)
        if a < 2 * cl:
            first = h * cl + a if a < cl else oh * cl + (a - cl)
            s = jnp.where(lax.broadcasted_iota(jnp.int32, (e - a, 1), 0) < pref - first, s, NEG)
        else:
            key = lax.broadcasted_iota(jnp.int32, (e - a, cols), 0)
            tok = lax.broadcasted_iota(jnp.int32, (e - a, cols), 1) // grp
            s = jnp.where(key - tok <= (chip - x) * (2 * toks), s, NEG)
        dst[a:e, :] = s
        mb = jnp.max(s.reshape((e - a) // 8, 8, cols), axis=0)
        return mb if mx is None else jnp.maximum(mx, mb)

    def value_chunk(k, a, e, src, mc, o, l):
        p = jnp.exp2(src[a:e, :] * c2 - mc)
        lsum = jnp.sum(p.reshape((e - a) // 8, 8, cols), axis=0)
        oo = jnp.dot(vb[k, :, a:e], p.astype(BF), preferred_element_type=F32)
        return (oo if o is None else o + oo), (lsum if l is None else l + lsum)

    def step(slot, cur, nxt, extra=None):
        mx = o = l = None
        if nxt is not None:
            k2, r2, b2 = nxt
            qv = qb[r2 * heads + k2].reshape(cols, dim)
            chip = chip_of(r2)
        if cur is not None:
            k, b1, u = cur
            mc = mscr[slot][0:1, :]
        count = max(len(b2) if nxt is not None else 0, len(b1) if cur is not None else 0)
        for i in range(count):
            if extra is not None and i == count // 3:
                extra()
            if nxt is not None and i < len(b2):
                mx = score_chunk(k2, qv, chip, *b2[i], S[1 - slot], mx)
            if cur is not None and i < len(b1):
                o, l = value_chunk(k, *b1[i], S[slot], mc, o, l)
        if nxt is not None:
            mscr[1 - slot] = jnp.broadcast_to(jnp.max(mx, axis=0, keepdims=True) * c2, (8, cols))
        if cur is not None:
            ls = jnp.sum(l, axis=0, keepdims=True)
            osend[u] = (o * (1.0 / ls)).T.astype(BF)
            lse = mc + jnp.log2(ls)
            lsend[u, 0] = lse[:, :rows]
            lsend[u, 1] = lse[:, rows:]

    def slot_of(k, c):
        return k * 3 + (c - 1)

    def own_slot(k, half):
        return heads * 3 + half * heads + k

    def piece(a):
        return pl.ds(pl.multiple_of(a * rows, 16), rows)

    def result(u, a, dst_o, dst_l, so, sl, chip, core):
        return (remote(osend.at[u, piece(a)], dst_o, oss, so, chip, core),
                remote(lsend.at[u, a], dst_l, lss, sl, chip, core))

    hh_of = lambda k: h * heads + k

    def own_copies(k, half):
        hh = hh_of(k)
        rel = 3 * half
        return result(own_slot(k, half), oh, ob.at[rel, hh], lb.at[rel, hh], ors.at[rel, hh], lrs.at[rel, hh], x, oh)

    def side_copies(k, c):
        hh = hh_of(k)
        if isinstance(c, int):
            a, rel, chip = (c - 1), 3 - c, chips[c]
        else:
            a, rel, chip = c - 1, 3 - c, pick(c, chips)
        return result(slot_of(k, c), a, ob.at[rel, hh], lb.at[rel, hh], ors.at[rel, hh], lrs.at[rel, hh], chip, a)

    def far_copies(k, a):
        chip = (xr, xl)[a]
        return result(slot_of(k, FAR), a, orel.at[a, k], lrel.at[a, k], rrs.at[a, k], rlr.at[a, k], chip, h)

    def merged_copies(k, a):
        hh = hh_of(k)
        chip, rel = ((xr, LEFT), (xl, RIGHT))[a]
        return (remote(orel.at[a, heads + k], ob.at[rel, hh], rss, ors.at[rel, hh], chip, a),
                remote(lrel.at[a, heads + k], lb.at[rel, hh], rls, lrs.at[rel, hh], chip, a))

    def columns(ws):
        pad = jnp.zeros((8 - len(ws), rows), F32)
        return jnp.concatenate(list(ws) + [pad], axis=0).T

    def relay_wait(k):
        for a in (0, 1):
            arrived(orel.at[a, k], rrs.at[a, k])
            arrived(lrel.at[a, k], rlr.at[a, k])

    def relay_merge(k):
        for a in (0, 1):
            u = slot_of(k, (RIGHT, LEFT)[a])
            l0, l1 = lsend[u, a], lrel[a, k]
            m = jnp.maximum(l0, l1)
            w0, w1 = jnp.exp2(l0 - m), jnp.exp2(l1 - m)
            tot = w0 + w1
            inv = 1.0 / tot
            wt = columns((w0 * inv, w1 * inv))
            orel[a, heads + k] = (osend[u, a * rows:(a + 1) * rows, :].astype(F32) * wt[:, 0:1]
                                  + orel[a, k].astype(F32) * wt[:, 1:2]).astype(BF)
            lrel[a, heads + k] = m + jnp.log2(tot)

    def relay_send(k):
        for a in (0, 1):
            for cp in merged_copies(k, a):
                cp.start()

    def start(cps):
        for cp in cps:
            cp.start()

    def wait_q(k, c):
        if isinstance(c, int):
            if c != LEFT:
                q_arrived(c, 0, k)
            if c != RIGHT:
                q_arrived(c, 1, k)
        else:
            @pl.when(c != LEFT)
            def _():
                q_arrived(c, 0, k)

            @pl.when(c != RIGHT)
            def _():
                q_arrived(c, 1, k)

    def send_unit(k, c):
        if isinstance(c, int):
            if c == FAR:
                start(far_copies(k, 0))
                start(far_copies(k, 1))
            else:
                start(side_copies(k, c))
        else:
            @pl.when(c == FAR)
            def _():
                start(far_copies(k, 0))
                start(far_copies(k, 1))

            @pl.when(c != FAR)
            def _():
                start(side_copies(k, c))

    for p in range(PARTS):
        for cp in kv_local(p):
            cp.wait()
        split_part(p * part)
    wait_q(0, 0)
    step(1, None, (0, 0, own_b))
    for k in range(heads - 1):
        wait_q(k + 1, 0)
        step(k % 2, (k, own_b, own_slot(k, 0)), (k + 1, 0, own_b))
        start(own_copies(k, 0))
        if k == 1:
            forwards(0)

    for cp in new_local():
        cp.wait()
    for i, st in enumerate((knst, vnst)):
        arrived(st.at[pl.ds(oh * toks, toks)], nvr.at[i])
    split(knst[...], vnst[...], 2 * toks, 2 * cl)
    for p in range(PARTS):
        kv_arrived(p)
        split_part(cl + p * part)
    forwards(1)
    wait_q(*UNITS[0])
    step((heads - 1) % 2, (heads - 1, own_b, own_slot(heads - 1, 0)), UNITS[0] + (all_b,))
    start(own_copies(heads - 1, 0))

    def go(u, k, c, k2, c2_, slot):
        wait_q(k2, c2_)
        step(slot, (k, all_b, slot_of(k, c)), (k2, c2_, all_b))
        send_unit(k, c)

    hs, cs = [u[0] for u in UNITS], [u[1] for u in UNITS]

    def pair(i, carry):
        u = 2 * i
        go(u, pick(u, hs), pick(u, cs), pick(u + 1, hs), pick(u + 1, cs), 0)

        @pl.when(i < 2)
        def _():
            forwards(2 + i)
        go(u + 1, pick(u + 1, hs), pick(u + 1, cs), pick(u + 2, hs), pick(u + 2, cs), 1)
        return carry

    lax.fori_loop(0, LOOPED // 2, pair, 0)
    rest = oth_b + new_b
    last = len(UNITS) - 1
    relays = {LOOPED: 0, LOOPED + 1: 1, LOOPED + 2: 2}
    for u in range(LOOPED, last + 1):
        k, c = UNITS[u]
        nxt = UNITS[u + 1] + (all_b,) if u < last else (0, 0, rest)
        if u < last:
            wait_q(*UNITS[u + 1])
        r = relays.get(u)
        if r is not None:
            relay_wait(r)
        step(u % 2, (k, all_b, slot_of(k, c)), nxt, None if r is None else functools.partial(relay_merge, r))
        send_unit(k, c)
        if r is not None:
            relay_send(r)

    def final(k, own):
        hh = (h if own else oh) * heads + k
        if own:
            parts = [(osend[own_slot(k, half), piece(h), :], lsend[own_slot(k, half), h]) for half in (0, 1)]
        else:
            parts = [(ob[rel, hh], lb[rel, hh]) for rel in (0, 3)]
        parts += [(ob[rel, hh], lb[rel, hh]) for rel in (LEFT, RIGHT)]
        ls = [p[1] for p in parts]
        m = jnp.maximum(jnp.maximum(ls[0], ls[1]), jnp.maximum(ls[2], ls[3]))
        w = [jnp.exp2(v - m) for v in ls]
        tot = (w[0] + w[1]) + (w[2] + w[3])
        inv = 1.0 / tot
        wt = columns([v * inv for v in w])
        acc = None
        for r in range(4):
            t = parts[r][0].astype(F32) * wt[:, r:r + 1]
            acc = t if acc is None else acc + t
        o_out[:, hh] = acc.astype(BF).reshape(toks, grp, dim)
        lfin[pl.ds(hh, 1), :] = (m + jnp.log2(tot)) * float(math.log(2.0))

    def final_wait(k):
        for own in (True, False):
            hh = (h if own else oh) * heads + k
            for rel in (LEFT, RIGHT) if own else (0, LEFT, RIGHT, 3):
                arrived(ob.at[rel, hh], ors.at[rel, hh])
                arrived(lb.at[rel, hh], lrs.at[rel, hh])

    def final_both(k):
        final(k, True)
        final(k, False)

    for k in range(heads):
        extra = None
        if k == 0:
            relay_wait(heads - 1)
            extra = functools.partial(relay_merge, heads - 1)
        elif k >= 2:
            final_wait(k - 2)
            extra = functools.partial(final_both, k - 2)
        step(k % 2, (k, rest, own_slot(k, 1)), (k + 1, 0, rest) if k + 1 < heads else None, extra)
        start(own_copies(k, 1))
        if k == 0:
            relay_send(heads - 1)
    for k in range(heads - 2, heads):
        final_wait(k)
    for k in range(heads - 2, heads):
        final_both(k)

    kh = 2 * heads
    ltr[...] = jnp.concatenate([lfin[...], jnp.zeros((128 - kh, rows), F32)], axis=0).T
    lse = None
    for g in range(grp):
        one = (lax.broadcasted_iota(jnp.int32, (128, kh * grp), 0) * grp + g == lax.broadcasted_iota(jnp.int32, (128, kh * grp), 1))
        t = jnp.dot(ltr[pl.ds(g, toks, stride=grp), :], one.astype(F32), preferred_element_type=F32, precision=lax.Precision.HIGHEST)
        lse = t if lse is None else lse + t
    l_out[...] = lse

    for buf, sem in ((qb.at[0:7 * heads // 2], qss), (osend.at[0:3 * heads], oss), (lsend.at[0:3 * heads], lss),
                     (orel.at[0], rss), (lrel.at[0], rls), (kst.at[0:cl], kvs.at[0]), (vst.at[0:cl], kvs.at[1])):
        arrived(buf, sem)
    for cp in new_remote():
        cp.wait_send()


def solution(mesh):
    n = mesh.shape['cp']
    tok = P(('dp', 'cp'))

    def local(queries, key_new, value_new, key_cache, value_cache, prefix_len):
        t, qh, d = queries.shape
        cl, kh = key_cache.shape[0], key_cache.shape[1]
        g = qh // kh
        hv = kh // 2
        rows = t * g
        nkeys = 2 * cl + 2 * t
        width = -(-nkeys // 128) * 128
        q = queries.reshape(t, 2, hv, g, d)
        kc, vc = (a.reshape(cl, 2, hv, d) for a in (key_cache, value_cache))
        kn, vn = (a.reshape(t, 2, hv, d) for a in (key_new, value_new))
        anyspec = pl.BlockSpec(memory_space=pltpu.HBM)
        vm = pl.BlockSpec(memory_space=pltpu.VMEM)
        dma = pltpu.SemaphoreType.DMA
        nres = 5 * hv
        o, l = pl.pallas_call(
            functools.partial(attend_kernel, n, d ** -0.5),
            name='attend',
            out_shape=(jax.ShapeDtypeStruct((t, kh, g, d), BF), jax.ShapeDtypeStruct((t, qh), F32)),
            in_specs=[pl.BlockSpec(memory_space=pltpu.SMEM)] + [anyspec] * 5,
            out_specs=(vm, vm),
            scratch_shapes=[
                pltpu.VMEM((hv, nkeys, d), BF),
                pltpu.VMEM((hv, d, width), BF),
                pltpu.VMEM((2 * cl, hv, d), BF),
                pltpu.VMEM((2 * cl, hv, d), BF),
                pltpu.VMEM((2 * t, hv, d), BF),
                pltpu.VMEM((2 * t, hv, d), BF),
                pltpu.VMEM((2, PREP * hv, d), F32),
                pltpu.VMEM((4 * hv, 2 * t, g, d), BF),
                pltpu.VMEM((4, kh, rows, d), BF),
                pltpu.VMEM((4, kh, 1, rows), F32),
                pltpu.VMEM((nres, 2 * rows, d), BF),
                pltpu.VMEM((nres, 2, 1, rows), F32),
                pltpu.VMEM((2, 2 * hv, rows, d), BF),
                pltpu.VMEM((2, 2 * hv, 1, rows), F32),
                pltpu.VMEM((nkeys, 2 * rows), F32),
                pltpu.VMEM((nkeys, 2 * rows), F32),
                pltpu.VMEM((2, 8, 2 * rows), F32),
                pltpu.VMEM((kh, rows), F32),
                pltpu.VMEM((rows, 128), F32),
                dma((2, PARTS)), dma((2,)), dma((2, PARTS)),
                dma((2,)), dma((2,)), dma((2,)),
                dma, dma((4, 2, hv)),
                dma, dma((4, kh)), dma, dma((4, kh)),
                dma, dma((2, hv)), dma, dma((2, hv)),
            ],
            compiler_params=pltpu.CompilerParams(collective_id=0, has_side_effects=True,
                                                 vmem_limit_bytes=40 * 2 ** 20),
        )(prefix_len, q, kn, vn, kc, vc)
        return o.reshape(t, qh, d), l

    return jax.shard_map(local, mesh=mesh, in_specs=(tok, tok, tok, tok, tok, P('dp')), out_specs=(tok, tok), check_vma=False)
```

```python
import functools
import math

import jax
import jax.numpy as jnp
from jax import lax
from jax.experimental import pallas as pl
from jax.experimental.pallas import tpu as pltpu
from jax.sharding import PartitionSpec as P

MESH = pl.DeviceIdType.MESH
NEG = -1e30
CH = 256
PREP = 256
PARTS = 3
LOOPED = 8
BF = jnp.bfloat16
F32 = jnp.float32
LEFT, RIGHT, FAR = 1, 2, 3
UNITS = ((0, LEFT), (0, RIGHT), (1, LEFT), (1, RIGHT), (0, FAR), (1, FAR),
         (2, LEFT), (2, RIGHT), (2, FAR), (3, FAR), (3, LEFT), (3, RIGHT))


def pick(i, table):
    out = table[0]
    for j, v in enumerate(table[1:], 1):
        out = jnp.where(i == j, v, out)
    return out


def attend_kernel(n, scale, plen, q, kn, vn, kc, vc, o_out, l_out,
                  kb, vb, kst, vst, knst, vnst, prep, qb, ob, lb, osend, lsend, orel, lrel, s0, s1, mscr, lfin, ltr,
                  kvl, kvs, kvr, nvl, nvs, nvr, qss, qrs, oss, ors, lss, lrs, rss, rrs, rls, rlr):
    S = (s0, s1)
    toks, heads, grp, dim = q.shape[0], q.shape[2], q.shape[3], q.shape[4]
    rows = toks * grp
    cols = 2 * rows
    cl = kc.shape[0]
    c2 = float(scale * math.log2(math.e))
    nch = n // 2
    me = lax.axis_index('cp')
    x, h = me // 2, lax.rem(me, 2)
    oh = 1 - h
    xl, xr, xd = lax.rem(x + nch - 1, nch), lax.rem(x + 1, nch), lax.rem(x + 2, nch)
    chips = (x, xl, xr, xd)

    def chip_of(c):
        return chips[c] if isinstance(c, int) else pick(c, chips)

    def remote(src, dst, ss, rs, chip, core):
        return pltpu.make_async_remote_copy(src_ref=src, dst_ref=dst, send_sem=ss, recv_sem=rs,
                                            device_id={'cp': chip * 2 + core}, device_id_type=MESH)

    def arrived(dst, sem):
        pltpu.make_async_copy(dst, dst, sem).wait()

    bar = pltpu.get_barrier_semaphore()
    for j in range(1, n):
        pl.semaphore_signal(bar, inc=1, device_id={'cp': lax.rem(me + j, n)}, device_id_type=MESH)

    part = cl // PARTS

    def kv_local(p):
        src = pl.ds(p * part, part)
        return [pltpu.make_async_copy(a.at[src, h], st.at[src], kvl.at[i, p]) for i, (a, st) in enumerate(((kc, kst), (vc, vst)))]

    def kv_remote(p):
        src, dst = pl.ds(p * part, part), pl.ds(cl + p * part, part)
        return [remote(a.at[src, oh], st.at[dst], kvs.at[i], kvr.at[i, p], x, oh) for i, (a, st) in enumerate(((kc, kst), (vc, vst)))]

    def kv_arrived(p):
        dst = pl.ds(cl + p * part, part)
        for i, st in enumerate((kst, vst)):
            arrived(st.at[dst], kvr.at[i, p])

    nrow = pl.ds(h * toks, toks)

    def new_local():
        return [pltpu.make_async_copy(a.at[:, h], st.at[nrow], nvl.at[i]) for i, (a, st) in enumerate(((kn, knst), (vn, vnst)))]

    def new_remote():
        return [remote(a.at[:, oh], st.at[nrow], nvs.at[i], nvr.at[i], x, oh) for i, (a, st) in enumerate(((kn, knst), (vn, vnst)))]

    def q_local(k):
        return pltpu.make_async_copy(q.at[:, h, k], qb.at[k, nrow], qrs.at[0, h, k])

    def q_partner(k):
        return remote(q.at[:, oh, k], qb.at[k, nrow], qss, qrs.at[0, h, k], x, oh)

    def q_remote(k):
        out = []
        for chip, rel in ((xl, RIGHT), (xr, LEFT)):
            for core in (0, 1):
                out.append(remote(q.at[:, core, k], qb.at[rel * heads + k, nrow], qss, qrs.at[rel, h, k], chip, core))
        return out

    def q_arrived(rel, core, k):
        arrived(qb.at[rel * heads + k, pl.ds(core * toks, toks)], qrs.at[rel, core, k])

    def forward(k, way):
        rel, chip = ((LEFT, xr), (RIGHT, xl))[way]
        piece = pl.ds(way * toks, toks)
        return remote(qb.at[rel * heads + k, piece], qb.at[FAR * heads + k, piece], qss, qrs.at[FAR, way, k], chip, h)

    def forwards(k):
        for way, rel in ((0, LEFT), (1, RIGHT)):
            q_arrived(rel, way, k)
            forward(k, way).start()

    for p in range(PARTS):
        for cp in kv_local(p):
            cp.start()
    for cp in new_local():
        cp.start()
    for k in range(heads):
        q_local(k).start()
    pl.semaphore_wait(bar, n - 1)
    for k in range(heads):
        q_partner(k).start()
    for cp in new_remote():
        cp.start()
    for k in range(heads):
        for cp in q_remote(k):
            cp.start()
    for p in range(PARTS):
        for cp in kv_remote(p):
            cp.start()

    def split(kraw, vraw, count, base):
        prep[0, 0:count * heads] = kraw.reshape(count * heads, dim).astype(F32)
        prep[1, 0:count * heads] = vraw.reshape(count * heads, dim).astype(F32)
        for j in range(heads):
            kb[j, pl.ds(base, count), :] = prep[0, pl.ds(j, count, stride=heads), :].astype(BF)
            vb[j, :, pl.ds(base, count)] = prep[1, pl.ds(j, count, stride=heads), :].astype(BF).T

    def split_part(first):
        def go(i, carry):
            base = pl.multiple_of(first + i * PREP, PREP)
            split(kst[pl.ds(base, PREP)], vst[pl.ds(base, PREP)], PREP, base)
            return carry
        lax.fori_loop(0, part // PREP, go, 0)

    pref = plen[0] - x * (2 * cl)
    own_b = [(a, a + CH) for a in range(0, cl, CH)]
    oth_b = [(a, a + CH) for a in range(cl, 2 * cl, CH)]
    new_b = [(2 * cl, 2 * cl + 2 * toks)]
    all_b = own_b + oth_b + new_b

    def score_chunk(k, qv, chip, a, e, dst, mx):
        s = lax.dot_general(kb[k, a:e, :], qv, (((1,), (1,)), ((), ())), preferred_element_type=F32)
        if a < 2 * cl:
            first = h * cl + a if a < cl else oh * cl + (a - cl)
            s = jnp.where(lax.broadcasted_iota(jnp.int32, (e - a, 1), 0) < pref - first, s, NEG)
        else:
            key = lax.broadcasted_iota(jnp.int32, (e - a, cols), 0)
            tok = lax.broadcasted_iota(jnp.int32, (e - a, cols), 1) // grp
            s = jnp.where(key - tok <= (chip - x) * (2 * toks), s, NEG)
        dst[a:e, :] = s
        mb = jnp.max(s.reshape((e - a) // 8, 8, cols), axis=0)
        return mb if mx is None else jnp.maximum(mx, mb)

    def value_chunk(k, a, e, src, mc, o, l):
        p = jnp.exp2(src[a:e, :] * c2 - mc)
        lsum = jnp.sum(p.reshape((e - a) // 8, 8, cols), axis=0)
        oo = jnp.dot(vb[k, :, a:e], p.astype(BF), preferred_element_type=F32)
        return (oo if o is None else o + oo), (lsum if l is None else l + lsum)

    def step(slot, cur, nxt, extra=None):
        mx = o = l = None
        if nxt is not None:
            k2, r2, b2 = nxt
            qv = qb[r2 * heads + k2].reshape(cols, dim)
            chip = chip_of(r2)
        if cur is not None:
            k, b1, u = cur
            mc = mscr[slot][0:1, :]
        count = max(len(b2) if nxt is not None else 0, len(b1) if cur is not None else 0)
        for i in range(count):
            if extra is not None and i == count // 3:
                extra()
            if nxt is not None and i < len(b2):
                mx = score_chunk(k2, qv, chip, *b2[i], S[1 - slot], mx)
            if cur is not None and i < len(b1):
                o, l = value_chunk(k, *b1[i], S[slot], mc, o, l)
        if nxt is not None:
            mscr[1 - slot] = jnp.broadcast_to(jnp.max(mx, axis=0, keepdims=True) * c2, (8, cols))
        if cur is not None:
            ls = jnp.sum(l, axis=0, keepdims=True)
            osend[u] = (o * (1.0 / ls)).T.astype(BF)
            lse = mc + jnp.log2(ls)
            lsend[u, 0] = lse[:, :rows]
            lsend[u, 1] = lse[:, rows:]

    def slot_of(k, c):
        return k * 3 + (c - 1)

    def own_slot(k, half):
        return heads * 3 + half * heads + k

    def piece(a):
        return pl.ds(pl.multiple_of(a * rows, 16), rows)

    def result(u, a, dst_o, dst_l, so, sl, chip, core):
        return (remote(osend.at[u, piece(a)], dst_o, oss, so, chip, core),
                remote(lsend.at[u, a], dst_l, lss, sl, chip, core))

    hh_of = lambda k: h * heads + k

    def own_copies(k, half):
        hh = hh_of(k)
        rel = 3 * half
        return result(own_slot(k, half), oh, ob.at[rel, hh], lb.at[rel, hh], ors.at[rel, hh], lrs.at[rel, hh], x, oh)

    def side_copies(k, c):
        hh = hh_of(k)
        if isinstance(c, int):
            a, rel, chip = (c - 1), 3 - c, chips[c]
        else:
            a, rel, chip = c - 1, 3 - c, pick(c, chips)
        return result(slot_of(k, c), a, ob.at[rel, hh], lb.at[rel, hh], ors.at[rel, hh], lrs.at[rel, hh], chip, a)

    def far_copies(k, a):
        chip = (xr, xl)[a]
        return result(slot_of(k, FAR), a, orel.at[a, k], lrel.at[a, k], rrs.at[a, k], rlr.at[a, k], chip, h)

    def merged_copies(k, a):
        hh = hh_of(k)
        chip, rel = ((xr, LEFT), (xl, RIGHT))[a]
        return (remote(orel.at[a, heads + k], ob.at[rel, hh], rss, ors.at[rel, hh], chip, a),
                remote(lrel.at[a, heads + k], lb.at[rel, hh], rls, lrs.at[rel, hh], chip, a))

    def columns(ws):
        pad = jnp.zeros((8 - len(ws), rows), F32)
        return jnp.concatenate(list(ws) + [pad], axis=0).T

    def relay_wait(k):
        for a in (0, 1):
            arrived(orel.at[a, k], rrs.at[a, k])
            arrived(lrel.at[a, k], rlr.at[a, k])

    def relay_merge(k):
        for a in (0, 1):
            u = slot_of(k, (RIGHT, LEFT)[a])
            l0, l1 = lsend[u, a], lrel[a, k]
            m = jnp.maximum(l0, l1)
            w0, w1 = jnp.exp2(l0 - m), jnp.exp2(l1 - m)
            tot = w0 + w1
            inv = 1.0 / tot
            wt = columns((w0 * inv, w1 * inv))
            orel[a, heads + k] = (osend[u, a * rows:(a + 1) * rows, :].astype(F32) * wt[:, 0:1]
                                  + orel[a, k].astype(F32) * wt[:, 1:2]).astype(BF)
            lrel[a, heads + k] = m + jnp.log2(tot)

    def relay_send(k):
        for a in (0, 1):
            for cp in merged_copies(k, a):
                cp.start()

    def start(cps):
        for cp in cps:
            cp.start()

    def wait_q(k, c):
        if isinstance(c, int):
            if c != LEFT:
                q_arrived(c, 0, k)
            if c != RIGHT:
                q_arrived(c, 1, k)
        else:
            @pl.when(c != LEFT)
            def _():
                q_arrived(c, 0, k)

            @pl.when(c != RIGHT)
            def _():
                q_arrived(c, 1, k)

    def send_unit(k, c):
        if isinstance(c, int):
            if c == FAR:
                start(far_copies(k, 0))
                start(far_copies(k, 1))
            else:
                start(side_copies(k, c))
        else:
            @pl.when(c == FAR)
            def _():
                start(far_copies(k, 0))
                start(far_copies(k, 1))

            @pl.when(c != FAR)
            def _():
                start(side_copies(k, c))

    for p in range(PARTS):
        for cp in kv_local(p):
            cp.wait()
        split_part(p * part)
    wait_q(0, 0)
    step(1, None, (0, 0, own_b))
    for k in range(heads - 1):
        wait_q(k + 1, 0)
        step(k % 2, (k, own_b, own_slot(k, 0)), (k + 1, 0, own_b))
        start(own_copies(k, 0))
        if k == 1:
            forwards(0)

    for cp in new_local():
        cp.wait()
    for i, st in enumerate((knst, vnst)):
        arrived(st.at[pl.ds(oh * toks, toks)], nvr.at[i])
    split(knst[...], vnst[...], 2 * toks, 2 * cl)
    for p in range(PARTS):
        kv_arrived(p)
        split_part(cl + p * part)
    forwards(1)
    wait_q(*UNITS[0])
    step((heads - 1) % 2, (heads - 1, own_b, own_slot(heads - 1, 0)), UNITS[0] + (all_b,))
    start(own_copies(heads - 1, 0))

    def go(u, k, c, k2, c2_, slot):
        wait_q(k2, c2_)
        step(slot, (k, all_b, slot_of(k, c)), (k2, c2_, all_b))
        send_unit(k, c)

    hs, cs = [u[0] for u in UNITS], [u[1] for u in UNITS]

    def pair(i, carry):
        u = 2 * i
        go(u, pick(u, hs), pick(u, cs), pick(u + 1, hs), pick(u + 1, cs), 0)

        @pl.when(i < 2)
        def _():
            forwards(2 + i)
        go(u + 1, pick(u + 1, hs), pick(u + 1, cs), pick(u + 2, hs), pick(u + 2, cs), 1)
        return carry

    lax.fori_loop(0, LOOPED // 2, pair, 0)
    rest = oth_b + new_b
    last = len(UNITS) - 1
    relays = {LOOPED: 0, LOOPED + 1: 1, LOOPED + 2: 2}
    for u in range(LOOPED, last + 1):
        k, c = UNITS[u]
        nxt = UNITS[u + 1] + (all_b,) if u < last else (0, 0, rest)
        if u < last:
            wait_q(*UNITS[u + 1])
        r = relays.get(u)
        if r is not None:
            relay_wait(r)
        step(u % 2, (k, all_b, slot_of(k, c)), nxt, None if r is None else functools.partial(relay_merge, r))
        send_unit(k, c)
        if r is not None:
            relay_send(r)

    def final(k, own):
        hh = (h if own else oh) * heads + k
        if own:
            parts = [(osend[own_slot(k, half), piece(h), :], lsend[own_slot(k, half), h]) for half in (0, 1)]
        else:
            parts = [(ob[rel, hh], lb[rel, hh]) for rel in (0, 3)]
        parts += [(ob[rel, hh], lb[rel, hh]) for rel in (LEFT, RIGHT)]
        ls = [p[1] for p in parts]
        m = jnp.maximum(jnp.maximum(ls[0], ls[1]), jnp.maximum(ls[2], ls[3]))
        w = [jnp.exp2(v - m) for v in ls]
        tot = (w[0] + w[1]) + (w[2] + w[3])
        inv = 1.0 / tot
        wt = columns([v * inv for v in w])
        acc = None
        for r in range(4):
            t = parts[r][0].astype(F32) * wt[:, r:r + 1]
            acc = t if acc is None else acc + t
        o_out[:, hh] = acc.astype(BF).reshape(toks, grp, dim)
        lfin[pl.ds(hh, 1), :] = (m + jnp.log2(tot)) * float(math.log(2.0))

    def final_wait(k):
        for own in (True, False):
            hh = (h if own else oh) * heads + k
            for rel in (LEFT, RIGHT) if own else (0, LEFT, RIGHT, 3):
                arrived(ob.at[rel, hh], ors.at[rel, hh])
                arrived(lb.at[rel, hh], lrs.at[rel, hh])

    def final_both(k):
        final(k, True)
        final(k, False)

    for k in range(heads):
        extra = None
        if k == 0:
            relay_wait(heads - 1)
            extra = functools.partial(relay_merge, heads - 1)
        elif k >= 2:
            final_wait(k - 2)
            extra = functools.partial(final_both, k - 2)
        step(k % 2, (k, rest, own_slot(k, 1)), (k + 1, 0, rest) if k + 1 < heads else None, extra)
        start(own_copies(k, 1))
        if k == 0:
            relay_send(heads - 1)
    for k in range(heads - 2, heads):
        final_wait(k)
    for k in range(heads - 2, heads):
        final_both(k)

    kh = 2 * heads
    ltr[...] = jnp.concatenate([lfin[...], jnp.zeros((128 - kh, rows), F32)], axis=0).T
    lse = None
    for g in range(grp):
        one = (lax.broadcasted_iota(jnp.int32, (128, kh * grp), 0) * grp + g == lax.broadcasted_iota(jnp.int32, (128, kh * grp), 1))
        t = jnp.dot(ltr[pl.ds(g, toks, stride=grp), :], one.astype(F32), preferred_element_type=F32, precision=lax.Precision.HIGHEST)
        lse = t if lse is None else lse + t
    l_out[...] = lse

    for buf, sem in ((qb.at[0:7 * heads // 2], qss), (osend.at[0:3 * heads], oss), (lsend.at[0:3 * heads], lss),
                     (orel.at[0], rss), (lrel.at[0], rls), (kst.at[0:cl], kvs.at[0]), (vst.at[0:cl], kvs.at[1])):
        arrived(buf, sem)
    for cp in new_remote():
        cp.wait_send()


def solution(mesh):
    n = mesh.shape['cp']
    tok = P(('dp', 'cp'))

    def local(queries, key_new, value_new, key_cache, value_cache, prefix_len):
        t, qh, d = queries.shape
        cl, kh = key_cache.shape[0], key_cache.shape[1]
        g = qh // kh
        hv = kh // 2
        rows = t * g
        nkeys = 2 * cl + 2 * t
        width = -(-nkeys // 128) * 128
        q = queries.reshape(t, 2, hv, g, d)
        kc, vc = (a.reshape(cl, 2, hv, d) for a in (key_cache, value_cache))
        kn, vn = (a.reshape(t, 2, hv, d) for a in (key_new, value_new))
        anyspec = pl.BlockSpec(memory_space=pltpu.HBM)
        vm = pl.BlockSpec(memory_space=pltpu.VMEM)
        dma = pltpu.SemaphoreType.DMA
        nres = 5 * hv
        o, l = pl.pallas_call(
            functools.partial(attend_kernel, n, d ** -0.5),
            name='attend',
            out_shape=(jax.ShapeDtypeStruct((t, kh, g, d), BF), jax.ShapeDtypeStruct((t, qh), F32)),
            in_specs=[pl.BlockSpec(memory_space=pltpu.SMEM)] + [anyspec] * 5,
            out_specs=(vm, vm),
            scratch_shapes=[
                pltpu.VMEM((hv, nkeys, d), BF),
                pltpu.VMEM((hv, d, width), BF),
                pltpu.VMEM((2 * cl, hv, d), BF),
                pltpu.VMEM((2 * cl, hv, d), BF),
                pltpu.VMEM((2 * t, hv, d), BF),
                pltpu.VMEM((2 * t, hv, d), BF),
                pltpu.VMEM((2, PREP * hv, d), F32),
                pltpu.VMEM((4 * hv, 2 * t, g, d), BF),
                pltpu.VMEM((4, kh, rows, d), BF),
                pltpu.VMEM((4, kh, 1, rows), F32),
                pltpu.VMEM((nres, 2 * rows, d), BF),
                pltpu.VMEM((nres, 2, 1, rows), F32),
                pltpu.VMEM((2, 2 * hv, rows, d), BF),
                pltpu.VMEM((2, 2 * hv, 1, rows), F32),
                pltpu.VMEM((nkeys, 2 * rows), F32),
                pltpu.VMEM((nkeys, 2 * rows), F32),
                pltpu.VMEM((2, 8, 2 * rows), F32),
                pltpu.VMEM((kh, rows), F32),
                pltpu.VMEM((rows, 128), F32),
                dma((2, PARTS)), dma((2,)), dma((2, PARTS)),
                dma((2,)), dma((2,)), dma((2,)),
                dma, dma((4, 2, hv)),
                dma, dma((4, kh)), dma, dma((4, kh)),
                dma, dma((2, hv)), dma, dma((2, hv)),
            ],
            compiler_params=pltpu.CompilerParams(collective_id=0, has_side_effects=True,
                                                 vmem_limit_bytes=40 * 2 ** 20),
        )(prefix_len, *[pltpu.with_memory_space_constraint(a, pltpu.HBM) for a in (q, kn, vn, kc, vc)])
        return o.reshape(t, qh, d), l

    return jax.shard_map(local, mesh=mesh, in_specs=(tok, tok, tok, tok, tok, P('dp')), out_specs=(tok, tok), check_vma=False)
```

```python
import functools
import math

import jax
import jax.numpy as jnp
from jax import lax
from jax.experimental import pallas as pl
from jax.experimental.pallas import tpu as pltpu
from jax.sharding import PartitionSpec as P

MESH = pl.DeviceIdType.MESH
NEG = -1e30
CH = 256
PREP = 256
PARTS = 3
BF = jnp.bfloat16
F32 = jnp.float32
LEFT, RIGHT, FAR = 1, 2, 3
def attend_kernel(n, scale, plen, q, kn, vn, kc, vc, o_out, l_out,
                  kb, vb, kst, vst, knst, vnst, prep, qb, ob, lb, osend, lsend, orel, lrel, s0, s1, mscr, lfin, ltr, lim, oacc, lacc,
                  kvl, kvs, kvr, nvl, nvs, nvr, qss, qrs, oss, ors, lss, lrs, rss, rrs, rls, rlr):
    S = (s0, s1)
    toks, heads, grp, dim = q.shape[0], q.shape[2], q.shape[3], q.shape[4]
    rows = toks * grp
    cols = 2 * rows
    cl = kc.shape[0]
    c2 = float(scale * math.log2(math.e))
    nch = n // 2
    me = lax.axis_index('cp')
    x, h = me // 2, lax.rem(me, 2)
    oh = 1 - h
    xl, xr, xd = lax.rem(x + nch - 1, nch), lax.rem(x + 1, nch), lax.rem(x + 2, nch)
    chips = (x, xl, xr, xd)

    def remote(src, dst, ss, rs, chip, core):
        return pltpu.make_async_remote_copy(src_ref=src, dst_ref=dst, send_sem=ss, recv_sem=rs,
                                            device_id={'cp': chip * 2 + core}, device_id_type=MESH)

    def arrived(dst, sem):
        pltpu.make_async_copy(dst, dst, sem).wait()

    bar = pltpu.get_barrier_semaphore()
    for j in range(1, n):
        pl.semaphore_signal(bar, inc=1, device_id={'cp': lax.rem(me + j, n)}, device_id_type=MESH)

    part = cl // PARTS

    def kv_local(p):
        src = pl.ds(p * part, part)
        return [pltpu.make_async_copy(a.at[src, h], st.at[src], kvl.at[i, p]) for i, (a, st) in enumerate(((kc, kst), (vc, vst)))]

    def kv_remote(p):
        src, dst = pl.ds(p * part, part), pl.ds(cl + p * part, part)
        return [remote(a.at[src, oh], st.at[dst], kvs.at[i], kvr.at[i, p], x, oh) for i, (a, st) in enumerate(((kc, kst), (vc, vst)))]

    def kv_arrived(p):
        dst = pl.ds(cl + p * part, part)
        for i, st in enumerate((kst, vst)):
            arrived(st.at[dst], kvr.at[i, p])

    nrow = pl.ds(h * toks, toks)

    def new_local():
        return [pltpu.make_async_copy(a.at[:, h], st.at[nrow], nvl.at[i]) for i, (a, st) in enumerate(((kn, knst), (vn, vnst)))]

    def new_remote():
        return [remote(a.at[:, oh], st.at[nrow], nvs.at[i], nvr.at[i], x, oh) for i, (a, st) in enumerate(((kn, knst), (vn, vnst)))]

    def q_local(k):
        return pltpu.make_async_copy(q.at[:, h, k], qb.at[k, nrow], qrs.at[0, h, k])

    def q_partner(k):
        return remote(q.at[:, oh, k], qb.at[k, nrow], qss, qrs.at[0, h, k], x, oh)

    def q_remote(k):
        out = []
        for chip, rel in ((xl, RIGHT), (xr, LEFT)):
            for core in (0, 1):
                out.append(remote(q.at[:, core, k], qb.at[rel * heads + k, nrow], qss, qrs.at[rel, h, k], chip, core))
        return out

    def q_arrived(rel, core, k):
        arrived(qb.at[rel * heads + k, pl.ds(core * toks, toks)], qrs.at[rel, core, k])

    def forward(k, way):
        rel, chip = ((LEFT, xr), (RIGHT, xl))[way]
        piece = pl.ds(way * toks, toks)
        return remote(qb.at[rel * heads + k, piece], qb.at[FAR * heads + k, piece], qss, qrs.at[FAR, way, k], chip, h)

    def forwards(k):
        for way, rel in ((0, LEFT), (1, RIGHT)):
            q_arrived(rel, way, k)
            forward(k, way).start()
        if k + heads // 2 < heads:
            for cp in q_remote(k + heads // 2):
                cp.start()

    for p in range(PARTS):
        for cp in kv_local(p):
            cp.start()
    for cp in new_local():
        cp.start()
    for k in range(heads):
        q_local(k).start()
    pl.semaphore_wait(bar, n - 1)
    for k in range(heads):
        q_partner(k).start()
    for cp in new_remote():
        cp.start()
    for k in range(heads // 2):
        for cp in q_remote(k):
            cp.start()
    for p in range(PARTS):
        for cp in kv_remote(p):
            cp.start()

    pref = plen[0] - x * (2 * cl)

    def split(kraw, vraw, count, base, valid=None):
        prep[0, 0:count * heads] = kraw.reshape(count * heads, dim).astype(F32)
        prep[1, 0:count * heads] = vraw.reshape(count * heads, dim).astype(F32)

        def rows_of(w, j):
            v = prep[w, pl.ds(j, count, stride=heads), :]
            if valid is not None:
                v = jnp.where(lax.broadcasted_iota(jnp.int32, (count, 1), 0) < valid, v, 0.0)
            return v.astype(BF)

        for j in range(heads):
            kb[j, pl.ds(base, count), :] = rows_of(0, j)
            vb[j, :, pl.ds(base, count)] = rows_of(1, j).T

    def split_part(first, start_pos):
        for may_hide in (False, True):
            @pl.when(4 * (x + 1) > 3 * nch if may_hide else 4 * (x + 1) <= 3 * nch)
            def _(may_hide=may_hide):
                def go(i, carry):
                    base = pl.multiple_of(first + i * PREP, PREP)
                    valid = pref - (start_pos + i * PREP)
                    split(kst[pl.ds(base, PREP)], vst[pl.ds(base, PREP)], PREP, base, valid if may_hide else None)
                    lim[pl.ds(base, PREP), :] = jnp.where(lax.broadcasted_iota(jnp.int32, (PREP, 128), 0) < valid, float(jnp.finfo(F32).max), NEG)
                    return carry
                lax.fori_loop(0, part // PREP, go, 0)

    own_b = [(a, a + CH) for a in range(0, cl, CH)]
    oth_b = [(a, a + CH) for a in range(cl, 2 * cl, CH)]
    new_b = [(2 * cl, 2 * cl + 2 * toks)]
    all_b = own_b + oth_b + new_b

    def score_chunk(k, qv, chip, a, e, dst, mx):
        s = lax.dot_general(kb[k, a:e, :], qv, (((1,), (1,)), ((), ())), preferred_element_type=F32)
        if a < 2 * cl:
            s = jnp.minimum(s, jnp.concatenate([lim[a:e, :]] * (cols // 128), axis=1))
        else:
            key = lax.broadcasted_iota(jnp.int32, (e - a, cols), 0)
            tok = lax.broadcasted_iota(jnp.int32, (e - a, cols), 1) // grp
            s = jnp.where(key - tok <= (chip - x) * (2 * toks), s, NEG)
        dst[a:e, :] = s
        mb = jnp.max(s.reshape((e - a) // 8, 8, cols), axis=0)
        return mb if mx is None else jnp.maximum(mx, mb)

    def value_chunk(k, a, e, src, mc, o, l):
        p = jnp.exp2(src[a:e, :] * c2 - mc)
        lsum = jnp.sum(p.reshape((e - a) // 8, 8, cols), axis=0)
        pp = p.astype(BF)
        if cols % 256:
            pp = jnp.concatenate([pp, pp[:, :256 - cols % 256]], axis=1)
        oo = jnp.dot(vb[k, :, a:e], pp, preferred_element_type=F32)
        return (oo if o is None else o + oo), (lsum if l is None else l + lsum)

    def step(slot, cur, nxt, extras=()):
        mx = o = l = None
        if nxt is not None:
            k2, r2, b2 = nxt
            qv = qb[r2 * heads + k2].reshape(cols, dim)
        if cur is not None:
            k, b1 = cur
            mc = mscr[slot][0:1, :]
        count = max(len(b2) if nxt is not None else 0, len(b1) if cur is not None else 0)
        for i in range(count):
            if nxt is not None and i < len(b2):
                mx = score_chunk(k2, qv, chips[r2], *b2[i], S[1 - slot], mx)
            if cur is not None and i < len(b1):
                o, l = value_chunk(k, *b1[i], S[slot], mc, o, l)
            for j, extra in enumerate(extras):
                if i == min(1 + 2 * j, count - 1):
                    extra()
        if nxt is not None:
            mscr[1 - slot] = jnp.broadcast_to(jnp.max(mx, axis=0, keepdims=True) * c2, (8, cols))
        if cur is not None:
            ls = jnp.sum(l, axis=0, keepdims=True)
            oacc[slot] = o[:, :cols]
            lacc[slot, 0:1] = 1.0 / ls
            lacc[slot, 1:2] = mc + jnp.log2(ls)

    def close(u, slot):
        osend[u] = (oacc[slot] * lacc[slot, 0:1]).T.astype(BF)
        lse = lacc[slot, 1:2]
        lsend[u, 0] = lse[:, :rows]
        lsend[u, 1] = lse[:, rows:]

    def slot_of(k, c):
        return k * 3 + (c - 1)

    def own_slot(k, half):
        return heads * 3 + half * heads + k

    def piece(a):
        return pl.ds(pl.multiple_of(a * rows, 16), rows)

    def result(u, a, dst_o, dst_l, so, sl, chip, core):
        return (remote(osend.at[u, piece(a)], dst_o, oss, so, chip, core),
                remote(lsend.at[u, a], dst_l, lss, sl, chip, core))

    hh_of = lambda k: h * heads + k

    def own_copies(k, half):
        hh = hh_of(k)
        rel = 3 * half
        return result(own_slot(k, half), oh, ob.at[rel, hh], lb.at[rel, hh], ors.at[rel, hh], lrs.at[rel, hh], x, oh)

    def side_copies(k, c):
        hh = hh_of(k)
        a, rel, chip = (c - 1), 3 - c, chips[c]
        return result(slot_of(k, c), a, ob.at[rel, hh], lb.at[rel, hh], ors.at[rel, hh], lrs.at[rel, hh], chip, a)

    def far_copies(k, a):
        chip = (xr, xl)[a]
        return result(slot_of(k, FAR), a, orel.at[a, k], lrel.at[a, k], rrs.at[a, k], rlr.at[a, k], chip, h)

    def merged_copies(k, a):
        hh = hh_of(k)
        chip, rel = ((xr, LEFT), (xl, RIGHT))[a]
        return (remote(orel.at[a, heads + k], ob.at[rel, hh], rss, ors.at[rel, hh], chip, a),
                remote(lrel.at[a, heads + k], lb.at[rel, hh], rls, lrs.at[rel, hh], chip, a))

    def columns(ws):
        pad = jnp.zeros((8 - len(ws), rows), F32)
        return jnp.concatenate(list(ws) + [pad], axis=0).T

    def relay_wait(k):
        for a in (0, 1):
            arrived(orel.at[a, k], rrs.at[a, k])
            arrived(lrel.at[a, k], rlr.at[a, k])

    def relay_merge(k):
        for a in (0, 1):
            u = slot_of(k, (RIGHT, LEFT)[a])
            l0, l1 = lsend[u, a], lrel[a, k]
            m = jnp.maximum(l0, l1)
            w0, w1 = jnp.exp2(l0 - m), jnp.exp2(l1 - m)
            tot = w0 + w1
            inv = 1.0 / tot
            wt = columns((w0 * inv, w1 * inv))
            orel[a, heads + k] = (osend[u, a * rows:(a + 1) * rows, :].astype(F32) * wt[:, 0:1]
                                  + orel[a, k].astype(F32) * wt[:, 1:2]).astype(BF)
            lrel[a, heads + k] = m + jnp.log2(tot)

    def relay_send(k):
        for a in (0, 1):
            for cp in merged_copies(k, a):
                cp.start()

    def start(cps):
        for cp in cps:
            cp.start()

    def wait_q(k, c):
        if c != LEFT:
            q_arrived(c, 0, k)
        if c != RIGHT:
            q_arrived(c, 1, k)

    for p in range(PARTS):
        for cp in kv_local(p):
            cp.wait()
        split_part(p * part, h * cl + p * part)

    def other_keys():
        for cp in new_local():
            cp.wait()
        for i, st in enumerate((knst, vnst)):
            arrived(st.at[pl.ds(oh * toks, toks)], nvr.at[i])
        split(knst[...], vnst[...], 2 * toks, 2 * cl)
        for p in range(PARTS):
            kv_arrived(p)
            split_part(cl + p * part, oh * cl + p * part)

    def final(k, own):
        hh = (h if own else oh) * heads + k
        if own:
            parts = [(osend[own_slot(k, half), piece(h), :], lsend[own_slot(k, half), h]) for half in (0, 1)]
        else:
            parts = [(ob[rel, hh], lb[rel, hh]) for rel in (0, 3)]
        parts += [(ob[rel, hh], lb[rel, hh]) for rel in (LEFT, RIGHT)]
        ls = [p[1] for p in parts]
        m = jnp.maximum(jnp.maximum(ls[0], ls[1]), jnp.maximum(ls[2], ls[3]))
        w = [jnp.exp2(v - m) for v in ls]
        tot = (w[0] + w[1]) + (w[2] + w[3])
        inv = 1.0 / tot
        wt = columns([v * inv for v in w])
        acc = None
        for r in range(4):
            t = parts[r][0].astype(F32) * wt[:, r:r + 1]
            acc = t if acc is None else acc + t
        o_out[:, hh] = acc.astype(BF).reshape(toks, grp, dim)
        lfin[pl.ds(hh, 1), :] = (m + jnp.log2(tot)) * float(math.log(2.0))

    def final_wait(k):
        for own in (True, False):
            hh = (h if own else oh) * heads + k
            for rel in (LEFT, RIGHT) if own else (0, LEFT, RIGHT, 3):
                arrived(ob.at[rel, hh], ors.at[rel, hh])
                arrived(lb.at[rel, hh], lrs.at[rel, hh])

    def final_both(k):
        final(k, True)
        final(k, False)

    rest = oth_b + new_b
    units = [(k, 0, own_b, own_slot(k, 0)) for k in range(heads)]
    for k in range(heads):
        units += [(k, c, all_b, slot_of(k, c)) for c in (FAR, LEFT, RIGHT)]
    units += [(k, 0, rest, own_slot(k, 1)) for k in range(heads)]
    nown, total = heads, len(units)
    before = {1: [functools.partial(forwards, 0)], nown - 1: [other_keys, functools.partial(forwards, 1)]}
    for k in range(2, heads):
        before.setdefault(nown + 3 * (k - 2) + 1, []).append(functools.partial(forwards, k))
    merge_at = {nown + 3 * k + 5: k for k in range(heads - 1)}
    merge_at[total - heads + 1] = heads - 1

    def send(i):
        k, c, b, u = units[i]
        if c == 0:
            start(own_copies(k, 0 if i < nown else 1))
        elif c == FAR:
            start(far_copies(k, 0))
            start(far_copies(k, 1))
        else:
            start(side_copies(k, c))

    wait_q(0, 0)
    step(1, None, (0, 0, own_b))
    for i in range(total):
        for f in before.get(i, ()):
            f()
        k, c, b, u = units[i]
        nxt = None
        if i + 1 < total:
            k2, c2_, b2, _ = units[i + 1]
            if not (c2_ == 0 and i + 1 >= nown):
                wait_q(k2, c2_)
            nxt = (k2, c2_, b2)
        extras = []
        if i > 0:
            extras.append(functools.partial(close, units[i - 1][3], (i - 1) % 2))
        r = merge_at.get(i)
        if r is not None:
            relay_wait(r)
            extras.append(functools.partial(relay_merge, r))
        if i == total - 1:
            final_wait(0)
            extras.append(functools.partial(final_both, 0))
        step(i % 2, (k, b), nxt, extras)
        if i > 0:
            send(i - 1)
        if r is not None:
            relay_send(r)
    final_wait(1)
    close(units[-1][3], (total - 1) % 2)
    final_both(1)
    send(total - 1)
    for k in range(2, heads):
        final_wait(k)
        final_both(k)

    kh = 2 * heads
    ltr[...] = jnp.concatenate([lfin[...], jnp.zeros((128 - kh, rows), F32)], axis=0).T
    lse = None
    for g in range(grp):
        one = (lax.broadcasted_iota(jnp.int32, (128, kh * grp), 0) * grp + g == lax.broadcasted_iota(jnp.int32, (128, kh * grp), 1))
        t = jnp.dot(ltr[pl.ds(g, toks, stride=grp), :], one.astype(F32), preferred_element_type=F32, precision=lax.Precision.HIGHEST)
        lse = t if lse is None else lse + t
    l_out[...] = lse

    for buf, sem in ((qb.at[0:7 * heads // 2], qss), (osend.at[0:3 * heads], oss), (lsend.at[0:3 * heads], lss),
                     (orel.at[0], rss), (lrel.at[0], rls), (kst.at[0:cl], kvs.at[0]), (vst.at[0:cl], kvs.at[1])):
        arrived(buf, sem)
    for cp in new_remote():
        cp.wait_send()


def solution(mesh):
    n = mesh.shape['cp']
    tok = P(('dp', 'cp'))

    def local(queries, key_new, value_new, key_cache, value_cache, prefix_len):
        t, qh, d = queries.shape
        cl, kh = key_cache.shape[0], key_cache.shape[1]
        g = qh // kh
        hv = kh // 2
        rows = t * g
        nkeys = 2 * cl + 2 * t
        width = -(-nkeys // 128) * 128
        q = queries.reshape(t, 2, hv, g, d)
        kc, vc = (a.reshape(cl, 2, hv, d) for a in (key_cache, value_cache))
        kn, vn = (a.reshape(t, 2, hv, d) for a in (key_new, value_new))
        anyspec = pl.BlockSpec(memory_space=pltpu.HBM)
        vm = pl.BlockSpec(memory_space=pltpu.VMEM)
        dma = pltpu.SemaphoreType.DMA
        nres = 5 * hv
        o, l = pl.pallas_call(
            functools.partial(attend_kernel, n, d ** -0.5),
            name='attend',
            out_shape=(jax.ShapeDtypeStruct((t, kh, g, d), BF), jax.ShapeDtypeStruct((t, qh), F32)),
            in_specs=[pl.BlockSpec(memory_space=pltpu.SMEM)] + [anyspec] * 5,
            out_specs=(vm, vm),
            scratch_shapes=[
                pltpu.VMEM((hv, nkeys, d), BF),
                pltpu.VMEM((hv, d, width), BF),
                pltpu.VMEM((2 * cl, hv, d), BF),
                pltpu.VMEM((2 * cl, hv, d), BF),
                pltpu.VMEM((2 * t, hv, d), BF),
                pltpu.VMEM((2 * t, hv, d), BF),
                pltpu.VMEM((2, PREP * hv, d), F32),
                pltpu.VMEM((4 * hv, 2 * t, g, d), BF),
                pltpu.VMEM((4, kh, rows, d), BF),
                pltpu.VMEM((4, kh, 1, rows), F32),
                pltpu.VMEM((nres, 2 * rows, d), BF),
                pltpu.VMEM((nres, 2, 1, rows), F32),
                pltpu.VMEM((2, 2 * hv, rows, d), BF),
                pltpu.VMEM((2, 2 * hv, 1, rows), F32),
                pltpu.VMEM((nkeys, 2 * rows), F32),
                pltpu.VMEM((nkeys, 2 * rows), F32),
                pltpu.VMEM((2, 8, 2 * rows), F32),
                pltpu.VMEM((kh, rows), F32),
                pltpu.VMEM((rows, 128), F32),
                pltpu.VMEM((2 * cl, 128), F32),
                pltpu.VMEM((2, d, 2 * rows), F32),
                pltpu.VMEM((2, 8, 2 * rows), F32),
                dma((2, PARTS)), dma((2,)), dma((2, PARTS)),
                dma((2,)), dma((2,)), dma((2,)),
                dma, dma((4, 2, hv)),
                dma, dma((4, kh)), dma, dma((4, kh)),
                dma, dma((2, hv)), dma, dma((2, hv)),
            ],
            compiler_params=pltpu.CompilerParams(collective_id=0, has_side_effects=True,
                                                 vmem_limit_bytes=40 * 2 ** 20),
        )(prefix_len, *[pltpu.with_memory_space_constraint(a, pltpu.HBM) for a in (q, kn, vn, kc, vc)])
        return o.reshape(t, qh, d), l

    return jax.shard_map(local, mesh=mesh, in_specs=(tok, tok, tok, tok, tok, P('dp')), out_specs=(tok, tok), check_vma=False)
```

```python
import functools
import math

import jax
import jax.numpy as jnp
from jax import lax
from jax.experimental import pallas as pl
from jax.experimental.pallas import tpu as pltpu
from jax.sharding import PartitionSpec as P

MESH = pl.DeviceIdType.MESH
NEG = -1e30
CH = 256
PREP = 256
PARTS = 3
BF = jnp.bfloat16
F32 = jnp.float32
LEFT, RIGHT, FAR = 1, 2, 3
ORDER = ((0, LEFT), (0, RIGHT), (0, FAR), (1, FAR), (1, LEFT), (1, RIGHT),
         (2, FAR), (3, FAR), (2, LEFT), (2, RIGHT), (3, LEFT), (3, RIGHT))
def attend_kernel(n, scale, plen, q, kn, vn, kc, vc, o_out, l_out,
                  kb, vb, kst, vst, knst, vnst, prep, qb, ob, lb, osend, lsend, orel, lrel, s0, s1, mscr, lfin, ltr, lim, oacc, lacc,
                  kvl, kvs, kvr, nvl, nvs, nvr, qss, qrs, oss, ors, lss, lrs, rss, rrs, rls, rlr):
    S = (s0, s1)
    toks, heads, grp, dim = q.shape[0], q.shape[2], q.shape[3], q.shape[4]
    rows = toks * grp
    cols = 2 * rows
    cl = kc.shape[0]
    c2 = float(scale * math.log2(math.e))
    nch = n // 2
    me = lax.axis_index('cp')
    x, h = me // 2, lax.rem(me, 2)
    oh = 1 - h
    xl, xr, xd = lax.rem(x + nch - 1, nch), lax.rem(x + 1, nch), lax.rem(x + 2, nch)
    chips = (x, xl, xr, xd)

    def remote(src, dst, ss, rs, chip, core):
        return pltpu.make_async_remote_copy(src_ref=src, dst_ref=dst, send_sem=ss, recv_sem=rs,
                                            device_id={'cp': chip * 2 + core}, device_id_type=MESH)

    def arrived(dst, sem):
        pltpu.make_async_copy(dst, dst, sem).wait()

    bar = pltpu.get_barrier_semaphore()
    for j in range(1, n):
        pl.semaphore_signal(bar, inc=1, device_id={'cp': lax.rem(me + j, n)}, device_id_type=MESH)

    part = cl // PARTS

    def kv_local(p):
        src = pl.ds(p * part, part)
        return [pltpu.make_async_copy(a.at[src, h], st.at[src], kvl.at[i, p]) for i, (a, st) in enumerate(((kc, kst), (vc, vst)))]

    def kv_remote(p):
        src, dst = pl.ds(p * part, part), pl.ds(cl + p * part, part)
        return [remote(a.at[src, oh], st.at[dst], kvs.at[i], kvr.at[i, p], x, oh) for i, (a, st) in enumerate(((kc, kst), (vc, vst)))]

    def kv_arrived(p):
        dst = pl.ds(cl + p * part, part)
        for i, st in enumerate((kst, vst)):
            arrived(st.at[dst], kvr.at[i, p])

    nrow = pl.ds(h * toks, toks)

    def new_local():
        return [pltpu.make_async_copy(a.at[:, h], st.at[nrow], nvl.at[i]) for i, (a, st) in enumerate(((kn, knst), (vn, vnst)))]

    def new_remote():
        return [remote(a.at[:, oh], st.at[nrow], nvs.at[i], nvr.at[i], x, oh) for i, (a, st) in enumerate(((kn, knst), (vn, vnst)))]

    def q_local(k):
        return pltpu.make_async_copy(q.at[:, h, k], qb.at[k, nrow], qrs.at[0, h, k])

    def q_partner(k):
        return remote(q.at[:, oh, k], qb.at[k, nrow], qss, qrs.at[0, h, k], x, oh)

    def q_remote(k):
        out = []
        for chip, rel in ((xl, RIGHT), (xr, LEFT)):
            for core in (0, 1):
                out.append(remote(q.at[:, core, k], qb.at[rel * heads + k, nrow], qss, qrs.at[rel, h, k], chip, core))
        return out

    def q_arrived(rel, core, k):
        arrived(qb.at[rel * heads + k, pl.ds(core * toks, toks)], qrs.at[rel, core, k])

    def forward(k, way):
        rel, chip = ((LEFT, xr), (RIGHT, xl))[way]
        piece = pl.ds(way * toks, toks)
        return remote(qb.at[rel * heads + k, piece], qb.at[FAR * heads + k, piece], qss, qrs.at[FAR, way, k], chip, h)

    def forwards(k):
        for way, rel in ((0, LEFT), (1, RIGHT)):
            q_arrived(rel, way, k)
            forward(k, way).start()
        if k + heads // 2 < heads:
            for cp in q_remote(k + heads // 2):
                cp.start()

    for p in range(PARTS):
        for cp in kv_local(p):
            cp.start()
    for cp in new_local():
        cp.start()
    for k in range(heads):
        q_local(k).start()
    pl.semaphore_wait(bar, n - 1)
    for k in range(heads):
        q_partner(k).start()
    for cp in new_remote():
        cp.start()
    for k in range(heads // 2):
        for cp in q_remote(k):
            cp.start()
    for p in range(PARTS):
        for cp in kv_remote(p):
            cp.start()

    pref = plen[0] - x * (2 * cl)

    def split(kraw, vraw, count, base, valid=None):
        prep[0, 0:count * heads] = kraw.reshape(count * heads, dim).astype(F32)
        prep[1, 0:count * heads] = vraw.reshape(count * heads, dim).astype(F32)

        def rows_of(w, j):
            v = prep[w, pl.ds(j, count, stride=heads), :]
            if valid is not None:
                v = jnp.where(lax.broadcasted_iota(jnp.int32, (count, 1), 0) < valid, v, 0.0)
            return v.astype(BF)

        for j in range(heads):
            kb[j, pl.ds(base, count), :] = rows_of(0, j)
            vb[j, :, pl.ds(base, count)] = rows_of(1, j).T

    def split_part(first, start_pos):
        for may_hide in (False, True):
            @pl.when(4 * (x + 1) > 3 * nch if may_hide else 4 * (x + 1) <= 3 * nch)
            def _(may_hide=may_hide):
                def go(i, carry):
                    base = pl.multiple_of(first + i * PREP, PREP)
                    valid = pref - (start_pos + i * PREP)
                    split(kst[pl.ds(base, PREP)], vst[pl.ds(base, PREP)], PREP, base, valid if may_hide else None)
                    lim[pl.ds(base, PREP), :] = jnp.where(lax.broadcasted_iota(jnp.int32, (PREP, 128), 0) < valid, float(jnp.finfo(F32).max), NEG)
                    return carry
                lax.fori_loop(0, part // PREP, go, 0)

    own_b = [(a, a + CH) for a in range(0, cl, CH)]
    oth_b = [(a, a + CH) for a in range(cl, 2 * cl, CH)]
    new_b = [(2 * cl, 2 * cl + 2 * toks)]
    all_b = own_b + oth_b + new_b

    def score_chunk(k, qv, chip, a, e, dst, mx):
        s = lax.dot_general(kb[k, a:e, :], qv, (((1,), (1,)), ((), ())), preferred_element_type=F32)
        if a < 2 * cl:
            s = jnp.minimum(s, jnp.concatenate([lim[a:e, :]] * (cols // 128), axis=1))
        else:
            key = lax.broadcasted_iota(jnp.int32, (e - a, cols), 0)
            tok = lax.broadcasted_iota(jnp.int32, (e - a, cols), 1) // grp
            s = jnp.where(key - tok <= (chip - x) * (2 * toks), s, NEG)
        dst[a:e, :] = s
        mb = jnp.max(s.reshape((e - a) // 8, 8, cols), axis=0)
        return mb if mx is None else jnp.maximum(mx, mb)

    def value_chunk(k, a, e, src, mc, o, l):
        p = jnp.exp2(src[a:e, :] * c2 - mc)
        lsum = jnp.sum(p.reshape((e - a) // 8, 8, cols), axis=0)
        pp = p.astype(BF)
        if cols % 256:
            pp = jnp.concatenate([pp, pp[:, :256 - cols % 256]], axis=1)
        oo = jnp.dot(vb[k, :, a:e], pp, preferred_element_type=F32)
        return (oo if o is None else o + oo), (lsum if l is None else l + lsum)

    def step(slot, cur, nxt, extras=()):
        mx = o = l = None
        if nxt is not None:
            k2, r2, b2 = nxt
            qv = qb[r2 * heads + k2].reshape(cols, dim)
        if cur is not None:
            k, b1 = cur
            mc = mscr[slot][0:1, :]
        count = max(len(b2) if nxt is not None else 0, len(b1) if cur is not None else 0)
        for i in range(count):
            if nxt is not None and i < len(b2):
                mx = score_chunk(k2, qv, chips[r2], *b2[i], S[1 - slot], mx)
            if cur is not None and i < len(b1):
                o, l = value_chunk(k, *b1[i], S[slot], mc, o, l)
            for j, extra in enumerate(extras):
                if i == min(1 + 2 * j, count - 1):
                    extra()
        if nxt is not None:
            mscr[1 - slot] = jnp.broadcast_to(jnp.max(mx, axis=0, keepdims=True) * c2, (8, cols))
        if cur is not None:
            ls = jnp.sum(l, axis=0, keepdims=True)
            oacc[slot] = o[:, :cols]
            lacc[slot, 0:1] = 1.0 / ls
            lacc[slot, 1:2] = mc + jnp.log2(ls)

    def close(u, slot):
        osend[u] = (oacc[slot] * lacc[slot, 0:1]).T.astype(BF)
        lse = lacc[slot, 1:2]
        lsend[u, 0] = lse[:, :rows]
        lsend[u, 1] = lse[:, rows:]

    def slot_of(k, c):
        return k * 3 + (c - 1)

    def own_slot(k, half):
        return heads * 3 + half * heads + k

    def piece(a):
        return pl.ds(pl.multiple_of(a * rows, 16), rows)

    def result(u, a, dst_o, dst_l, so, sl, chip, core):
        return (remote(osend.at[u, piece(a)], dst_o, oss, so, chip, core),
                remote(lsend.at[u, a], dst_l, lss, sl, chip, core))

    hh_of = lambda k: h * heads + k

    def own_copies(k, half):
        hh = hh_of(k)
        rel = 3 * half
        return result(own_slot(k, half), oh, ob.at[rel, hh], lb.at[rel, hh], ors.at[rel, hh], lrs.at[rel, hh], x, oh)

    def side_copies(k, c):
        hh = hh_of(k)
        a, rel, chip = (c - 1), 3 - c, chips[c]
        return result(slot_of(k, c), a, ob.at[rel, hh], lb.at[rel, hh], ors.at[rel, hh], lrs.at[rel, hh], chip, a)

    def far_copies(k, a):
        chip = (xr, xl)[a]
        return result(slot_of(k, FAR), a, orel.at[a, k], lrel.at[a, k], rrs.at[a, k], rlr.at[a, k], chip, h)

    def merged_copies(k, a):
        hh = hh_of(k)
        chip, rel = ((xr, LEFT), (xl, RIGHT))[a]
        return (remote(orel.at[a, heads + k], ob.at[rel, hh], rss, ors.at[rel, hh], chip, a),
                remote(lrel.at[a, heads + k], lb.at[rel, hh], rls, lrs.at[rel, hh], chip, a))

    def columns(ws):
        pad = jnp.zeros((8 - len(ws), rows), F32)
        return jnp.concatenate(list(ws) + [pad], axis=0).T

    def relay_wait(k):
        for a in (0, 1):
            arrived(orel.at[a, k], rrs.at[a, k])
            arrived(lrel.at[a, k], rlr.at[a, k])

    def relay_merge(k):
        for a in (0, 1):
            u = slot_of(k, (RIGHT, LEFT)[a])
            l0, l1 = lsend[u, a], lrel[a, k]
            m = jnp.maximum(l0, l1)
            w0, w1 = jnp.exp2(l0 - m), jnp.exp2(l1 - m)
            tot = w0 + w1
            inv = 1.0 / tot
            wt = columns((w0 * inv, w1 * inv))
            orel[a, heads + k] = (osend[u, a * rows:(a + 1) * rows, :].astype(F32) * wt[:, 0:1]
                                  + orel[a, k].astype(F32) * wt[:, 1:2]).astype(BF)
            lrel[a, heads + k] = m + jnp.log2(tot)

    def relay_send(k):
        for a in (0, 1):
            for cp in merged_copies(k, a):
                cp.start()

    def start(cps):
        for cp in cps:
            cp.start()

    def wait_q(k, c):
        if c != LEFT:
            q_arrived(c, 0, k)
        if c != RIGHT:
            q_arrived(c, 1, k)

    for p in range(PARTS):
        for cp in kv_local(p):
            cp.wait()
        split_part(p * part, h * cl + p * part)

    def other_keys():
        for cp in new_local():
            cp.wait()
        for i, st in enumerate((knst, vnst)):
            arrived(st.at[pl.ds(oh * toks, toks)], nvr.at[i])
        split(knst[...], vnst[...], 2 * toks, 2 * cl)
        for p in range(PARTS):
            kv_arrived(p)
            split_part(cl + p * part, oh * cl + p * part)

    def final(k, own):
        hh = (h if own else oh) * heads + k
        if own:
            parts = [(osend[own_slot(k, half), piece(h), :], lsend[own_slot(k, half), h]) for half in (0, 1)]
        else:
            parts = [(ob[rel, hh], lb[rel, hh]) for rel in (0, 3)]
        parts += [(ob[rel, hh], lb[rel, hh]) for rel in (LEFT, RIGHT)]
        ls = [p[1] for p in parts]
        m = jnp.maximum(jnp.maximum(ls[0], ls[1]), jnp.maximum(ls[2], ls[3]))
        w = [jnp.exp2(v - m) for v in ls]
        tot = (w[0] + w[1]) + (w[2] + w[3])
        inv = 1.0 / tot
        wt = columns([v * inv for v in w])
        acc = None
        for r in range(4):
            t = parts[r][0].astype(F32) * wt[:, r:r + 1]
            acc = t if acc is None else acc + t
        o_out[:, hh] = acc.astype(BF).reshape(toks, grp, dim)
        lfin[pl.ds(hh, 1), :] = (m + jnp.log2(tot)) * float(math.log(2.0))

    def final_wait(k):
        for own in (True, False):
            hh = (h if own else oh) * heads + k
            for rel in (LEFT, RIGHT) if own else (0, LEFT, RIGHT, 3):
                arrived(ob.at[rel, hh], ors.at[rel, hh])
                arrived(lb.at[rel, hh], lrs.at[rel, hh])

    def final_both(k):
        final(k, True)
        final(k, False)

    rest = oth_b + new_b
    units = [(k, 0, own_b, own_slot(k, 0)) for k in range(heads)]
    units += [(k, c, all_b, slot_of(k, c)) for k, c in ORDER]
    units += [(k, 0, rest, own_slot(k, 1)) for k in range(heads)]
    nown, total = heads, len(units)
    before = {2: [functools.partial(forwards, 0)], nown - 1: [other_keys, functools.partial(forwards, 1)]}
    for k in range(2, heads):
        before.setdefault(nown + k - 1, []).append(functools.partial(forwards, k))
    merge_at = {10: 0, 12: 1, 15: 2, 17: 3}

    def send(i):
        k, c, b, u = units[i]
        if c == 0:
            start(own_copies(k, 0 if i < nown else 1))
        elif c == FAR:
            start(far_copies(k, 0))
            start(far_copies(k, 1))
        else:
            start(side_copies(k, c))

    wait_q(0, 0)
    step(1, None, (0, 0, own_b))
    for i in range(total):
        for f in before.get(i, ()):
            f()
        k, c, b, u = units[i]
        nxt = None
        if i + 1 < total:
            k2, c2_, b2, _ = units[i + 1]
            if not (c2_ == 0 and i + 1 >= nown):
                wait_q(k2, c2_)
            nxt = (k2, c2_, b2)
        extras = []
        if i > 0:
            extras.append(functools.partial(close, units[i - 1][3], (i - 1) % 2))
        r = merge_at.get(i)
        if r is not None:
            relay_wait(r)
            extras.append(functools.partial(relay_merge, r))
        if i == total - 1:
            final_wait(0)
            extras.append(functools.partial(final_both, 0))
        step(i % 2, (k, b), nxt, extras)
        if i > 0:
            send(i - 1)
        if r is not None:
            relay_send(r)
    final_wait(1)
    close(units[-1][3], (total - 1) % 2)
    final_both(1)
    send(total - 1)
    for k in range(2, heads):
        final_wait(k)
    for k in range(2, heads):
        final_both(k)

    kh = 2 * heads
    ltr[...] = jnp.concatenate([lfin[...], jnp.zeros((128 - kh, rows), F32)], axis=0).T
    lse = None
    for g in range(grp):
        one = (lax.broadcasted_iota(jnp.int32, (128, kh * grp), 0) * grp + g == lax.broadcasted_iota(jnp.int32, (128, kh * grp), 1))
        t = jnp.dot(ltr[pl.ds(g, toks, stride=grp), :], one.astype(F32), preferred_element_type=F32, precision=lax.Precision.HIGHEST)
        lse = t if lse is None else lse + t
    l_out[...] = lse

    for buf, sem in ((qb.at[0:7 * heads // 2], qss), (osend.at[0:3 * heads], oss), (lsend.at[0:3 * heads], lss),
                     (orel.at[0], rss), (lrel.at[0], rls), (kst.at[0:cl], kvs.at[0]), (vst.at[0:cl], kvs.at[1])):
        arrived(buf, sem)
    for cp in new_remote():
        cp.wait_send()


def solution(mesh):
    n = mesh.shape['cp']
    tok = P(('dp', 'cp'))

    def local(queries, key_new, value_new, key_cache, value_cache, prefix_len):
        t, qh, d = queries.shape
        cl, kh = key_cache.shape[0], key_cache.shape[1]
        g = qh // kh
        hv = kh // 2
        rows = t * g
        nkeys = 2 * cl + 2 * t
        width = -(-nkeys // 128) * 128
        q = queries.reshape(t, 2, hv, g, d)
        kc, vc = (a.reshape(cl, 2, hv, d) for a in (key_cache, value_cache))
        kn, vn = (a.reshape(t, 2, hv, d) for a in (key_new, value_new))
        anyspec = pl.BlockSpec(memory_space=pltpu.HBM)
        vm = pl.BlockSpec(memory_space=pltpu.VMEM)
        dma = pltpu.SemaphoreType.DMA
        nres = 5 * hv
        o, l = pl.pallas_call(
            functools.partial(attend_kernel, n, d ** -0.5),
            name='attend',
            out_shape=(jax.ShapeDtypeStruct((t, kh, g, d), BF), jax.ShapeDtypeStruct((t, qh), F32)),
            in_specs=[pl.BlockSpec(memory_space=pltpu.SMEM)] + [anyspec] * 5,
            out_specs=(vm, vm),
            scratch_shapes=[
                pltpu.VMEM((hv, nkeys, d), BF),
                pltpu.VMEM((hv, d, width), BF),
                pltpu.VMEM((2 * cl, hv, d), BF),
                pltpu.VMEM((2 * cl, hv, d), BF),
                pltpu.VMEM((2 * t, hv, d), BF),
                pltpu.VMEM((2 * t, hv, d), BF),
                pltpu.VMEM((2, PREP * hv, d), F32),
                pltpu.VMEM((4 * hv, 2 * t, g, d), BF),
                pltpu.VMEM((4, kh, rows, d), BF),
                pltpu.VMEM((4, kh, 1, rows), F32),
                pltpu.VMEM((nres, 2 * rows, d), BF),
                pltpu.VMEM((nres, 2, 1, rows), F32),
                pltpu.VMEM((2, 2 * hv, rows, d), BF),
                pltpu.VMEM((2, 2 * hv, 1, rows), F32),
                pltpu.VMEM((nkeys, 2 * rows), F32),
                pltpu.VMEM((nkeys, 2 * rows), F32),
                pltpu.VMEM((2, 8, 2 * rows), F32),
                pltpu.VMEM((kh, rows), F32),
                pltpu.VMEM((rows, 128), F32),
                pltpu.VMEM((2 * cl, 128), F32),
                pltpu.VMEM((2, d, 2 * rows), F32),
                pltpu.VMEM((2, 8, 2 * rows), F32),
                dma((2, PARTS)), dma((2,)), dma((2, PARTS)),
                dma((2,)), dma((2,)), dma((2,)),
                dma, dma((4, 2, hv)),
                dma, dma((4, kh)), dma, dma((4, kh)),
                dma, dma((2, hv)), dma, dma((2, hv)),
            ],
            compiler_params=pltpu.CompilerParams(collective_id=0, has_side_effects=True,
                                                 vmem_limit_bytes=40 * 2 ** 20),
        )(prefix_len, *[pltpu.with_memory_space_constraint(a, pltpu.HBM) for a in (q, kn, vn, kc, vc)])
        return o.reshape(t, qh, d), l

    return jax.shard_map(local, mesh=mesh, in_specs=(tok, tok, tok, tok, tok, P('dp')), out_specs=(tok, tok), check_vma=False)
```

```python
import functools
import math

import jax
import jax.numpy as jnp
from jax import lax
from jax.experimental import pallas as pl
from jax.experimental.pallas import tpu as pltpu
from jax.sharding import PartitionSpec as P

MESH = pl.DeviceIdType.MESH
NEG = -1e30
CH = 256
PREP = 256
PARTS = 3
BF = jnp.bfloat16
F32 = jnp.float32
LEFT, RIGHT, FAR = 1, 2, 3
ORDER = ((0, LEFT), (0, RIGHT), (0, FAR), (1, FAR), (1, LEFT), (1, RIGHT),
         (2, FAR), (3, FAR), (2, LEFT), (2, RIGHT), (3, LEFT), (3, RIGHT))
def attend_kernel(n, scale, plen, q, kn, vn, kc, vc, o_out, l_out,
                  kb, vb, kst, vst, knst, vnst, prep, qb, ob, lb, osend, lsend, orel, lrel, s0, s1, mscr, lfin, ltr, lim, oacc, lacc,
                  kvl, kvs, kvr, nvl, nvs, nvr, qss, qrs, oss, ors, lss, lrs, rss, rrs, rls, rlr):
    S = (s0, s1)
    toks, heads, grp, dim = q.shape[0], q.shape[2], q.shape[3], q.shape[4]
    rows = toks * grp
    cols = 2 * rows
    cl = kc.shape[0]
    c2 = float(scale * math.log2(math.e))
    nch = n // 2
    me = lax.axis_index('cp')
    x, h = me // 2, lax.rem(me, 2)
    oh = 1 - h
    xl, xr, xd = lax.rem(x + nch - 1, nch), lax.rem(x + 1, nch), lax.rem(x + 2, nch)
    chips = (x, xl, xr, xd)

    def remote(src, dst, ss, rs, chip, core):
        return pltpu.make_async_remote_copy(src_ref=src, dst_ref=dst, send_sem=ss, recv_sem=rs,
                                            device_id={'cp': chip * 2 + core}, device_id_type=MESH)

    def arrived(dst, sem):
        pltpu.make_async_copy(dst, dst, sem).wait()

    bar = pltpu.get_barrier_semaphore()
    for j in range(1, n):
        pl.semaphore_signal(bar, inc=1, device_id={'cp': lax.rem(me + j, n)}, device_id_type=MESH)

    part = cl // PARTS

    def kv_local(p):
        src = pl.ds(p * part, part)
        return [pltpu.make_async_copy(a.at[src, h], st.at[src], kvl.at[i, p]) for i, (a, st) in enumerate(((kc, kst), (vc, vst)))]

    def kv_remote(p):
        src, dst = pl.ds(p * part, part), pl.ds(cl + p * part, part)
        return [remote(a.at[src, oh], st.at[dst], kvs.at[i], kvr.at[i, p], x, oh) for i, (a, st) in enumerate(((kc, kst), (vc, vst)))]

    def kv_arrived(p):
        dst = pl.ds(cl + p * part, part)
        for i, st in enumerate((kst, vst)):
            arrived(st.at[dst], kvr.at[i, p])

    nrow = pl.ds(h * toks, toks)

    def new_local():
        return [pltpu.make_async_copy(a.at[:, h], st.at[nrow], nvl.at[i]) for i, (a, st) in enumerate(((kn, knst), (vn, vnst)))]

    def new_remote():
        return [remote(a.at[:, oh], st.at[nrow], nvs.at[i], nvr.at[i], x, oh) for i, (a, st) in enumerate(((kn, knst), (vn, vnst)))]

    def q_local(k):
        return pltpu.make_async_copy(q.at[:, h, k], qb.at[k, nrow], qrs.at[0, h, k])

    def q_partner(k):
        return remote(q.at[:, oh, k], qb.at[k, nrow], qss, qrs.at[0, h, k], x, oh)

    def q_remote(k):
        out = []
        for chip, rel in ((xl, RIGHT), (xr, LEFT)):
            for core in (0, 1):
                out.append(remote(q.at[:, core, k], qb.at[rel * heads + k, nrow], qss, qrs.at[rel, h, k], chip, core))
        return out

    def q_arrived(rel, core, k):
        arrived(qb.at[rel * heads + k, pl.ds(core * toks, toks)], qrs.at[rel, core, k])

    def forward(k, way):
        rel, chip = ((LEFT, xr), (RIGHT, xl))[way]
        piece = pl.ds(way * toks, toks)
        return remote(qb.at[rel * heads + k, piece], qb.at[FAR * heads + k, piece], qss, qrs.at[FAR, way, k], chip, h)

    def forwards(k):
        for way, rel in ((0, LEFT), (1, RIGHT)):
            q_arrived(rel, way, k)
            forward(k, way).start()
        if k == 0:
            for cp in q_remote(heads - 1):
                cp.start()

    for p in range(PARTS):
        for cp in kv_local(p):
            cp.start()
    for cp in new_local():
        cp.start()
    for k in range(heads):
        q_local(k).start()
    pl.semaphore_wait(bar, n - 1)
    for k in range(heads):
        q_partner(k).start()
    for cp in new_remote():
        cp.start()
    for k in range(heads - 1):
        for cp in q_remote(k):
            cp.start()
    for p in range(PARTS):
        for cp in kv_remote(p):
            cp.start()

    pref = plen[0] - x * (2 * cl)

    def split(kraw, vraw, count, base, valid=None):
        prep[0, 0:count * heads] = kraw.reshape(count * heads, dim).astype(F32)
        prep[1, 0:count * heads] = vraw.reshape(count * heads, dim).astype(F32)

        def rows_of(w, j):
            v = prep[w, pl.ds(j, count, stride=heads), :]
            if valid is not None:
                v = jnp.where(lax.broadcasted_iota(jnp.int32, (count, 1), 0) < valid, v, 0.0)
            return v.astype(BF)

        for j in range(heads):
            kb[j, pl.ds(base, count), :] = rows_of(0, j)
            vb[j, :, pl.ds(base, count)] = rows_of(1, j).T

    def split_part(first, start_pos):
        for may_hide in (False, True):
            @pl.when(4 * (x + 1) > 3 * nch if may_hide else 4 * (x + 1) <= 3 * nch)
            def _(may_hide=may_hide):
                def go(i, carry):
                    base = pl.multiple_of(first + i * PREP, PREP)
                    valid = pref - (start_pos + i * PREP)
                    split(kst[pl.ds(base, PREP)], vst[pl.ds(base, PREP)], PREP, base, valid if may_hide else None)
                    lim[pl.ds(base, PREP), :] = jnp.where(lax.broadcasted_iota(jnp.int32, (PREP, 128), 0) < valid, float(jnp.finfo(F32).max), NEG)
                    return carry
                lax.fori_loop(0, part // PREP, go, 0)

    own_b = [(a, a + CH) for a in range(0, cl, CH)]
    oth_b = [(a, a + CH) for a in range(cl, 2 * cl, CH)]
    new_b = [(2 * cl, 2 * cl + 2 * toks)]
    all_b = own_b + oth_b + new_b

    def score_chunk(k, qv, chip, a, e, dst, mx):
        s = lax.dot_general(kb[k, a:e, :], qv, (((1,), (1,)), ((), ())), preferred_element_type=F32)
        if a < 2 * cl:
            s = jnp.minimum(s, jnp.concatenate([lim[a:e, :]] * (cols // 128), axis=1))
        else:
            key = lax.broadcasted_iota(jnp.int32, (e - a, cols), 0)
            tok = lax.broadcasted_iota(jnp.int32, (e - a, cols), 1) // grp
            s = jnp.where(key - tok <= (chip - x) * (2 * toks), s, NEG)
        dst[a:e, :] = s
        mb = jnp.max(s.reshape((e - a) // 8, 8, cols), axis=0)
        return mb if mx is None else jnp.maximum(mx, mb)

    def value_chunk(k, a, e, src, mc, o, l):
        p = jnp.exp2(src[a:e, :] * c2 - mc)
        lsum = jnp.sum(p.reshape((e - a) // 8, 8, cols), axis=0)
        pp = p.astype(BF)
        if cols % 256:
            pp = jnp.concatenate([pp, pp[:, :256 - cols % 256]], axis=1)
        oo = jnp.dot(vb[k, :, a:e], pp, preferred_element_type=F32)
        return (oo if o is None else o + oo), (lsum if l is None else l + lsum)

    def step(slot, cur, nxt, extras=()):
        mx = o = l = None
        if nxt is not None:
            k2, r2, b2 = nxt
            qv = qb[r2 * heads + k2].reshape(cols, dim)
        if cur is not None:
            k, b1 = cur
            mc = mscr[slot][0:1, :]
        count = max(len(b2) if nxt is not None else 0, len(b1) if cur is not None else 0)
        for i in range(count):
            if nxt is not None and i < len(b2):
                mx = score_chunk(k2, qv, chips[r2], *b2[i], S[1 - slot], mx)
            if cur is not None and i < len(b1):
                o, l = value_chunk(k, *b1[i], S[slot], mc, o, l)
            for j, extra in enumerate(extras):
                if i == min(1 + 2 * j, count - 1):
                    extra()
        if nxt is not None:
            mscr[1 - slot] = jnp.broadcast_to(jnp.max(mx, axis=0, keepdims=True) * c2, (8, cols))
        if cur is not None:
            ls = jnp.sum(l, axis=0, keepdims=True)
            oacc[slot] = o[:, :cols]
            lacc[slot, 0:1] = 1.0 / ls
            lacc[slot, 1:2] = mc + jnp.log2(ls)

    def close(u, slot):
        osend[u] = (oacc[slot] * lacc[slot, 0:1]).T.astype(BF)
        lse = lacc[slot, 1:2]
        lsend[u, 0] = lse[:, :rows]
        lsend[u, 1] = lse[:, rows:]

    def slot_of(k, c):
        return k * 3 + (c - 1)

    def own_slot(k, half):
        return heads * 3 + half * heads + k

    def piece(a):
        return pl.ds(pl.multiple_of(a * rows, 16), rows)

    def result(u, a, dst_o, dst_l, so, sl, chip, core):
        return (remote(osend.at[u, piece(a)], dst_o, oss, so, chip, core),
                remote(lsend.at[u, a], dst_l, lss, sl, chip, core))

    hh_of = lambda k: h * heads + k

    def own_copies(k, half):
        hh = hh_of(k)
        rel = 3 * half
        return result(own_slot(k, half), oh, ob.at[rel, hh], lb.at[rel, hh], ors.at[rel, hh], lrs.at[rel, hh], x, oh)

    def side_copies(k, c):
        hh = hh_of(k)
        a, rel, chip = (c - 1), 3 - c, chips[c]
        return result(slot_of(k, c), a, ob.at[rel, hh], lb.at[rel, hh], ors.at[rel, hh], lrs.at[rel, hh], chip, a)

    def far_copies(k, a):
        chip = (xr, xl)[a]
        return result(slot_of(k, FAR), a, orel.at[a, k], lrel.at[a, k], rrs.at[a, k], rlr.at[a, k], chip, h)

    def merged_copies(k, a):
        hh = hh_of(k)
        chip, rel = ((xr, LEFT), (xl, RIGHT))[a]
        return (remote(orel.at[a, heads + k], ob.at[rel, hh], rss, ors.at[rel, hh], chip, a),
                remote(lrel.at[a, heads + k], lb.at[rel, hh], rls, lrs.at[rel, hh], chip, a))

    def columns(ws):
        pad = jnp.zeros((8 - len(ws), rows), F32)
        return jnp.concatenate(list(ws) + [pad], axis=0).T

    def relay_wait(k):
        for a in (0, 1):
            arrived(orel.at[a, k], rrs.at[a, k])
            arrived(lrel.at[a, k], rlr.at[a, k])

    def relay_merge(k):
        for a in (0, 1):
            u = slot_of(k, (RIGHT, LEFT)[a])
            l0, l1 = lsend[u, a], lrel[a, k]
            m = jnp.maximum(l0, l1)
            w0, w1 = jnp.exp2(l0 - m), jnp.exp2(l1 - m)
            tot = w0 + w1
            inv = 1.0 / tot
            wt = columns((w0 * inv, w1 * inv))
            orel[a, heads + k] = (osend[u, a * rows:(a + 1) * rows, :].astype(F32) * wt[:, 0:1]
                                  + orel[a, k].astype(F32) * wt[:, 1:2]).astype(BF)
            lrel[a, heads + k] = m + jnp.log2(tot)

    def relay_send(k):
        for a in (0, 1):
            for cp in merged_copies(k, a):
                cp.start()

    def start(cps):
        for cp in cps:
            cp.start()

    def wait_q(k, c):
        if c != LEFT:
            q_arrived(c, 0, k)
        if c != RIGHT:
            q_arrived(c, 1, k)

    for p in range(PARTS):
        for cp in kv_local(p):
            cp.wait()
        split_part(p * part, h * cl + p * part)

    def other_keys():
        for cp in new_local():
            cp.wait()
        for i, st in enumerate((knst, vnst)):
            arrived(st.at[pl.ds(oh * toks, toks)], nvr.at[i])
        split(knst[...], vnst[...], 2 * toks, 2 * cl)
        for p in range(PARTS):
            kv_arrived(p)
            split_part(cl + p * part, oh * cl + p * part)

    def final(k, own):
        hh = (h if own else oh) * heads + k
        if own:
            parts = [(osend[own_slot(k, half), piece(h), :], lsend[own_slot(k, half), h]) for half in (0, 1)]
        else:
            parts = [(ob[rel, hh], lb[rel, hh]) for rel in (0, 3)]
        parts += [(ob[rel, hh], lb[rel, hh]) for rel in (LEFT, RIGHT)]
        ls = [p[1] for p in parts]
        m = jnp.maximum(jnp.maximum(ls[0], ls[1]), jnp.maximum(ls[2], ls[3]))
        w = [jnp.exp2(v - m) for v in ls]
        tot = (w[0] + w[1]) + (w[2] + w[3])
        inv = 1.0 / tot
        wt = columns([v * inv for v in w])
        acc = None
        for r in range(4):
            t = parts[r][0].astype(F32) * wt[:, r:r + 1]
            acc = t if acc is None else acc + t
        o_out[:, hh] = acc.astype(BF).reshape(toks, grp, dim)
        lfin[pl.ds(hh, 1), :] = (m + jnp.log2(tot)) * float(math.log(2.0))

    def final_wait(k):
        for own in (True, False):
            hh = (h if own else oh) * heads + k
            for rel in (LEFT, RIGHT) if own else (0, LEFT, RIGHT, 3):
                arrived(ob.at[rel, hh], ors.at[rel, hh])
                arrived(lb.at[rel, hh], lrs.at[rel, hh])

    def final_both(k):
        final(k, True)
        final(k, False)

    rest = oth_b + new_b
    units = [(k, 0, own_b, own_slot(k, 0)) for k in range(heads)]
    units += [(k, c, all_b, slot_of(k, c)) for k, c in ORDER]
    units += [(k, 0, rest, own_slot(k, 1)) for k in range(heads)]
    nown, total = heads, len(units)
    before = {nown - 1: [other_keys, functools.partial(forwards, 0), functools.partial(forwards, 1)]}
    for k in range(2, heads):
        before.setdefault(nown + 2 * k - 3, []).append(functools.partial(forwards, k))
    merge_at = {11: 0, 12: 1, 15: 2, 17: 3}

    def send(i):
        k, c, b, u = units[i]
        if c == 0:
            start(own_copies(k, 0 if i < nown else 1))
        elif c == FAR:
            start(far_copies(k, 0))
            start(far_copies(k, 1))
        else:
            start(side_copies(k, c))

    wait_q(0, 0)
    step(1, None, (0, 0, own_b))
    for i in range(total):
        for f in before.get(i, ()):
            f()
        k, c, b, u = units[i]
        nxt = None
        if i + 1 < total:
            k2, c2_, b2, _ = units[i + 1]
            if not (c2_ == 0 and i + 1 >= nown):
                wait_q(k2, c2_)
            nxt = (k2, c2_, b2)
        extras = []
        if i > 0:
            extras.append(functools.partial(close, units[i - 1][3], (i - 1) % 2))
        r = merge_at.get(i)
        if r is not None:
            relay_wait(r)
            extras.append(functools.partial(relay_merge, r))
        if i == total - 1:
            final_wait(0)
            extras.append(functools.partial(final_both, 0))
        step(i % 2, (k, b), nxt, extras)
        if i > 0:
            send(i - 1)
        if r is not None:
            relay_send(r)
    final_wait(1)
    close(units[-1][3], (total - 1) % 2)
    final_both(1)
    send(total - 1)
    for k in range(2, heads):
        final_wait(k)
    for k in range(2, heads):
        final_both(k)

    kh = 2 * heads
    ltr[...] = jnp.concatenate([lfin[...], jnp.zeros((128 - kh, rows), F32)], axis=0).T
    lse = None
    for g in range(grp):
        one = (lax.broadcasted_iota(jnp.int32, (128, kh * grp), 0) * grp + g == lax.broadcasted_iota(jnp.int32, (128, kh * grp), 1))
        t = jnp.dot(ltr[pl.ds(g, toks, stride=grp), :], one.astype(F32), preferred_element_type=F32, precision=lax.Precision.HIGHEST)
        lse = t if lse is None else lse + t
    l_out[...] = lse

    for buf, sem in ((qb.at[0:7 * heads // 2], qss), (osend.at[0:3 * heads], oss), (lsend.at[0:3 * heads], lss),
                     (orel.at[0], rss), (lrel.at[0], rls), (kst.at[0:cl], kvs.at[0]), (vst.at[0:cl], kvs.at[1])):
        arrived(buf, sem)
    for cp in new_remote():
        cp.wait_send()


def solution(mesh):
    n = mesh.shape['cp']
    tok = P(('dp', 'cp'))

    def local(queries, key_new, value_new, key_cache, value_cache, prefix_len):
        t, qh, d = queries.shape
        cl, kh = key_cache.shape[0], key_cache.shape[1]
        g = qh // kh
        hv = kh // 2
        rows = t * g
        nkeys = 2 * cl + 2 * t
        width = -(-nkeys // 128) * 128
        q = queries.reshape(t, 2, hv, g, d)
        kc, vc = (a.reshape(cl, 2, hv, d) for a in (key_cache, value_cache))
        kn, vn = (a.reshape(t, 2, hv, d) for a in (key_new, value_new))
        anyspec = pl.BlockSpec(memory_space=pltpu.HBM)
        vm = pl.BlockSpec(memory_space=pltpu.VMEM)
        dma = pltpu.SemaphoreType.DMA
        nres = 5 * hv
        o, l = pl.pallas_call(
            functools.partial(attend_kernel, n, d ** -0.5),
            name='attend',
            out_shape=(jax.ShapeDtypeStruct((t, kh, g, d), BF), jax.ShapeDtypeStruct((t, qh), F32)),
            in_specs=[pl.BlockSpec(memory_space=pltpu.SMEM)] + [anyspec] * 5,
            out_specs=(vm, vm),
            scratch_shapes=[
                pltpu.VMEM((hv, nkeys, d), BF),
                pltpu.VMEM((hv, d, width), BF),
                pltpu.VMEM((2 * cl, hv, d), BF),
                pltpu.VMEM((2 * cl, hv, d), BF),
                pltpu.VMEM((2 * t, hv, d), BF),
                pltpu.VMEM((2 * t, hv, d), BF),
                pltpu.VMEM((2, PREP * hv, d), F32),
                pltpu.VMEM((4 * hv, 2 * t, g, d), BF),
                pltpu.VMEM((4, kh, rows, d), BF),
                pltpu.VMEM((4, kh, 1, rows), F32),
                pltpu.VMEM((nres, 2 * rows, d), BF),
                pltpu.VMEM((nres, 2, 1, rows), F32),
                pltpu.VMEM((2, 2 * hv, rows, d), BF),
                pltpu.VMEM((2, 2 * hv, 1, rows), F32),
                pltpu.VMEM((nkeys, 2 * rows), F32),
                pltpu.VMEM((nkeys, 2 * rows), F32),
                pltpu.VMEM((2, 8, 2 * rows), F32),
                pltpu.VMEM((kh, rows), F32),
                pltpu.VMEM((rows, 128), F32),
                pltpu.VMEM((2 * cl, 128), F32),
                pltpu.VMEM((2, d, 2 * rows), F32),
                pltpu.VMEM((2, 8, 2 * rows), F32),
                dma((2, PARTS)), dma((2,)), dma((2, PARTS)),
                dma((2,)), dma((2,)), dma((2,)),
                dma, dma((4, 2, hv)),
                dma, dma((4, kh)), dma, dma((4, kh)),
                dma, dma((2, hv)), dma, dma((2, hv)),
            ],
            compiler_params=pltpu.CompilerParams(collective_id=0, has_side_effects=True,
                                                 vmem_limit_bytes=40 * 2 ** 20),
        )(prefix_len, *[pltpu.with_memory_space_constraint(a, pltpu.HBM) for a in (q, kn, vn, kc, vc)])
        return o.reshape(t, qh, d), l

    return jax.shard_map(local, mesh=mesh, in_specs=(tok, tok, tok, tok, tok, P('dp')), out_specs=(tok, tok), check_vma=False)
```

```python
import functools
import math

import jax
import jax.numpy as jnp
from jax import lax
from jax.experimental import pallas as pl
from jax.experimental.pallas import tpu as pltpu
from jax.sharding import PartitionSpec as P

MESH = pl.DeviceIdType.MESH
NEG = -1e30
CH = 256
PREP = 256
PARTS = 3
BF = jnp.bfloat16
F32 = jnp.float32
LEFT, RIGHT, FAR = 1, 2, 3
ORDER = ((0, LEFT), (0, RIGHT), (0, FAR), (1, FAR), (1, LEFT), (1, RIGHT),
         (2, FAR), (3, FAR), (2, LEFT), (2, RIGHT), (3, LEFT), (3, RIGHT))
def attend_kernel(n, scale, plen, q, kn, vn, kc, vc, o_out, l_out,
                  kb, vb, kst, vst, knst, vnst, prep, qb, ob, lb, osend, lsend, orel, lrel, s0, s1, mscr, lfin, ltr, lim, oacc, lacc,
                  kvl, kvs, kvr, nvl, nvs, nvr, qss, qrs, oss, ors, lss, lrs, rss, rrs, rls, rlr):
    S = (s0, s1)
    toks, heads, grp, dim = q.shape[0], q.shape[2], q.shape[3], q.shape[4]
    rows = toks * grp
    cols = 2 * rows
    cl = kc.shape[0]
    c2 = float(scale * math.log2(math.e))
    nch = n // 2
    me = lax.axis_index('cp')
    x, h = me // 2, lax.rem(me, 2)
    oh = 1 - h
    xl, xr, xd = lax.rem(x + nch - 1, nch), lax.rem(x + 1, nch), lax.rem(x + 2, nch)
    chips = (x, xl, xr, xd)

    def remote(src, dst, ss, rs, chip, core):
        return pltpu.make_async_remote_copy(src_ref=src, dst_ref=dst, send_sem=ss, recv_sem=rs,
                                            device_id={'cp': chip * 2 + core}, device_id_type=MESH)

    def arrived(dst, sem):
        pltpu.make_async_copy(dst, dst, sem).wait()

    bar = pltpu.get_barrier_semaphore()
    for j in range(1, n):
        pl.semaphore_signal(bar, inc=1, device_id={'cp': lax.rem(me + j, n)}, device_id_type=MESH)

    part = cl // PARTS

    def kv_local(p):
        src = pl.ds(p * part, part)
        return [pltpu.make_async_copy(a.at[src, h], st.at[src], kvl.at[i, p]) for i, (a, st) in enumerate(((kc, kst), (vc, vst)))]

    def kv_remote(p):
        src, dst = pl.ds(p * part, part), pl.ds(cl + p * part, part)
        return [remote(a.at[src, oh], st.at[dst], kvs.at[i], kvr.at[i, p], x, oh) for i, (a, st) in enumerate(((kc, kst), (vc, vst)))]

    def kv_arrived(p):
        dst = pl.ds(cl + p * part, part)
        for i, st in enumerate((kst, vst)):
            arrived(st.at[dst], kvr.at[i, p])

    nrow = pl.ds(h * toks, toks)

    def new_local():
        return [pltpu.make_async_copy(a.at[:, h], st.at[nrow], nvl.at[i]) for i, (a, st) in enumerate(((kn, knst), (vn, vnst)))]

    def new_remote():
        return [remote(a.at[:, oh], st.at[nrow], nvs.at[i], nvr.at[i], x, oh) for i, (a, st) in enumerate(((kn, knst), (vn, vnst)))]

    def q_local(k):
        return pltpu.make_async_copy(q.at[:, h, k], qb.at[k, nrow], qrs.at[0, h, k])

    def q_partner(k):
        return remote(q.at[:, oh, k], qb.at[k, nrow], qss, qrs.at[0, h, k], x, oh)

    def q_remote(k):
        out = []
        for chip, rel in ((xl, RIGHT), (xr, LEFT)):
            for core in (0, 1):
                out.append(remote(q.at[:, core, k], qb.at[rel * heads + k, nrow], qss, qrs.at[rel, h, k], chip, core))
        return out

    def q_arrived(rel, core, k):
        arrived(qb.at[rel * heads + k, pl.ds(core * toks, toks)], qrs.at[rel, core, k])

    def forward(k, way):
        rel, chip = ((LEFT, xr), (RIGHT, xl))[way]
        piece = pl.ds(way * toks, toks)
        return remote(qb.at[rel * heads + k, piece], qb.at[FAR * heads + k, piece], qss, qrs.at[FAR, way, k], chip, h)

    def forwards(k):
        for way, rel in ((0, LEFT), (1, RIGHT)):
            q_arrived(rel, way, k)
            forward(k, way).start()
        if k + heads // 2 < heads:
            for cp in q_remote(k + heads // 2):
                cp.start()

    for p in range(PARTS):
        for cp in kv_local(p):
            cp.start()
    for cp in new_local():
        cp.start()
    for k in range(heads):
        q_local(k).start()
    pl.semaphore_wait(bar, n - 1)
    for k in range(heads):
        q_partner(k).start()
    for cp in new_remote():
        cp.start()
    for k in range(heads // 2):
        for cp in q_remote(k):
            cp.start()
    for p in range(PARTS):
        for cp in kv_remote(p):
            cp.start()

    pref = plen[0] - x * (2 * cl)

    def split(kraw, vraw, count, base, valid=None):
        prep[0, 0:count * heads] = kraw.reshape(count * heads, dim).astype(F32)
        prep[1, 0:count * heads] = vraw.reshape(count * heads, dim).astype(F32)

        def rows_of(w, j):
            v = prep[w, pl.ds(j, count, stride=heads), :]
            if valid is not None:
                v = jnp.where(lax.broadcasted_iota(jnp.int32, (count, 1), 0) < valid, v, 0.0)
            return v.astype(BF)

        for j in range(heads):
            kb[j, pl.ds(base, count), :] = rows_of(0, j)
            vb[j, :, pl.ds(base, count)] = rows_of(1, j).T

    def split_part(first, start_pos):
        for may_hide in (False, True):
            @pl.when(4 * (x + 1) > 3 * nch if may_hide else 4 * (x + 1) <= 3 * nch)
            def _(may_hide=may_hide):
                def go(i, carry):
                    base = pl.multiple_of(first + i * PREP, PREP)
                    valid = pref - (start_pos + i * PREP)
                    split(kst[pl.ds(base, PREP)], vst[pl.ds(base, PREP)], PREP, base, valid if may_hide else None)
                    lim[pl.ds(base, PREP), :] = jnp.where(lax.broadcasted_iota(jnp.int32, (PREP, 128), 0) < valid, float(jnp.finfo(F32).max), NEG)
                    return carry
                lax.fori_loop(0, part // PREP, go, 0)

    own_b = [(a, a + CH) for a in range(0, cl, CH)]
    oth_b = [(a, a + CH) for a in range(cl, 2 * cl, CH)]
    new_b = [(2 * cl, 2 * cl + 2 * toks)]
    all_b = own_b + oth_b + new_b

    def score_chunk(k, qv, chip, a, e, dst, mx):
        s = lax.dot_general(kb[k, a:e, :], qv, (((1,), (1,)), ((), ())), preferred_element_type=F32)
        if a < 2 * cl:
            s = jnp.minimum(s, jnp.concatenate([lim[a:e, :]] * (cols // 128), axis=1))
        else:
            key = lax.broadcasted_iota(jnp.int32, (e - a, cols), 0)
            tok = lax.broadcasted_iota(jnp.int32, (e - a, cols), 1) // grp
            s = jnp.where(key - tok <= (chip - x) * (2 * toks), s, NEG)
        dst[a:e, :] = s
        mb = jnp.max(s.reshape((e - a) // 8, 8, cols), axis=0)
        return mb if mx is None else jnp.maximum(mx, mb)

    def value_chunk(k, a, e, src, mc, o, l):
        p = jnp.exp2(src[a:e, :] * c2 - mc)
        lsum = jnp.sum(p.reshape((e - a) // 8, 8, cols), axis=0)
        pp = p.astype(BF)
        if cols % 256:
            pp = jnp.concatenate([pp, pp[:, :256 - cols % 256]], axis=1)
        oo = jnp.dot(vb[k, :, a:e], pp, preferred_element_type=F32)
        return (oo if o is None else o + oo), (lsum if l is None else l + lsum)

    def step(slot, cur, nxt, extras=()):
        mx = o = l = None
        if nxt is not None:
            k2, r2, b2 = nxt
            qv = qb[r2 * heads + k2].reshape(cols, dim)
        if cur is not None:
            k, b1 = cur
            mc = mscr[slot][0:1, :]
        count = max(len(b2) if nxt is not None else 0, len(b1) if cur is not None else 0)
        for i in range(count):
            if nxt is not None and i < len(b2):
                mx = score_chunk(k2, qv, chips[r2], *b2[i], S[1 - slot], mx)
            if cur is not None and i < len(b1):
                o, l = value_chunk(k, *b1[i], S[slot], mc, o, l)
            for j, extra in enumerate(extras):
                if i == min(1 + 2 * j, count - 1):
                    extra()
        if nxt is not None:
            mscr[1 - slot] = jnp.broadcast_to(jnp.max(mx, axis=0, keepdims=True) * c2, (8, cols))
        if cur is not None:
            ls = jnp.sum(l, axis=0, keepdims=True)
            oacc[slot] = o[:, :cols]
            lacc[slot, 0:1] = 1.0 / ls
            lacc[slot, 1:2] = mc + jnp.log2(ls)

    def close(u, slot):
        osend[u] = (oacc[slot] * lacc[slot, 0:1]).T.astype(BF)
        lse = lacc[slot, 1:2]
        lsend[u, 0] = lse[:, :rows]
        lsend[u, 1] = lse[:, rows:]

    def slot_of(k, c):
        return k * 3 + (c - 1)

    def own_slot(k, half):
        return heads * 3 + half * heads + k

    def piece(a):
        return pl.ds(pl.multiple_of(a * rows, 16), rows)

    def result(u, a, dst_o, dst_l, so, sl, chip, core):
        return (remote(osend.at[u, piece(a)], dst_o, oss, so, chip, core),
                remote(lsend.at[u, a], dst_l, lss, sl, chip, core))

    hh_of = lambda k: h * heads + k

    def own_copies(k, half):
        hh = hh_of(k)
        rel = 3 * half
        return result(own_slot(k, half), oh, ob.at[rel, hh], lb.at[rel, hh], ors.at[rel, hh], lrs.at[rel, hh], x, oh)

    def side_copies(k, c):
        hh = hh_of(k)
        a, rel, chip = (c - 1), 3 - c, chips[c]
        return result(slot_of(k, c), a, ob.at[rel, hh], lb.at[rel, hh], ors.at[rel, hh], lrs.at[rel, hh], chip, a)

    def far_copies(k, a):
        chip = (xr, xl)[a]
        return result(slot_of(k, FAR), a, orel.at[a, k], lrel.at[a, k], rrs.at[a, k], rlr.at[a, k], chip, h)

    def merged_copies(k, a):
        hh = hh_of(k)
        chip, rel = ((xr, LEFT), (xl, RIGHT))[a]
        return (remote(orel.at[a, heads + k], ob.at[rel, hh], rss, ors.at[rel, hh], chip, a),
                remote(lrel.at[a, heads + k], lb.at[rel, hh], rls, lrs.at[rel, hh], chip, a))

    def columns(ws):
        pad = jnp.zeros((8 - len(ws), rows), F32)
        return jnp.concatenate(list(ws) + [pad], axis=0).T

    def relay_wait(k):
        for a in (0, 1):
            arrived(orel.at[a, k], rrs.at[a, k])
            arrived(lrel.at[a, k], rlr.at[a, k])

    def relay_merge(k):
        for a in (0, 1):
            u = slot_of(k, (RIGHT, LEFT)[a])
            l0, l1 = lsend[u, a], lrel[a, k]
            m = jnp.maximum(l0, l1)
            w0, w1 = jnp.exp2(l0 - m), jnp.exp2(l1 - m)
            tot = w0 + w1
            inv = 1.0 / tot
            wt = columns((w0 * inv, w1 * inv))
            orel[a, heads + k] = (osend[u, a * rows:(a + 1) * rows, :].astype(F32) * wt[:, 0:1]
                                  + orel[a, k].astype(F32) * wt[:, 1:2]).astype(BF)
            lrel[a, heads + k] = m + jnp.log2(tot)

    def relay_send(k):
        for a in (0, 1):
            for cp in merged_copies(k, a):
                cp.start()

    def start(cps):
        for cp in cps:
            cp.start()

    def wait_q(k, c):
        if c != LEFT:
            q_arrived(c, 0, k)
        if c != RIGHT:
            q_arrived(c, 1, k)

    for p in range(PARTS):
        for cp in kv_local(p):
            cp.wait()
        split_part(p * part, h * cl + p * part)

    def other_keys():
        for cp in new_local():
            cp.wait()
        for i, st in enumerate((knst, vnst)):
            arrived(st.at[pl.ds(oh * toks, toks)], nvr.at[i])
        split(knst[...], vnst[...], 2 * toks, 2 * cl)
        for p in range(PARTS):
            kv_arrived(p)
            split_part(cl + p * part, oh * cl + p * part)

    def final(k, own):
        hh = (h if own else oh) * heads + k
        if own:
            parts = [(osend[own_slot(k, half), piece(h), :], lsend[own_slot(k, half), h]) for half in (0, 1)]
        else:
            parts = [(ob[rel, hh], lb[rel, hh]) for rel in (0, 3)]
        parts += [(ob[rel, hh], lb[rel, hh]) for rel in (LEFT, RIGHT)]
        ls = [p[1] for p in parts]
        m = jnp.maximum(jnp.maximum(ls[0], ls[1]), jnp.maximum(ls[2], ls[3]))
        w = [jnp.exp2(v - m) for v in ls]
        tot = (w[0] + w[1]) + (w[2] + w[3])
        inv = 1.0 / tot
        wt = columns([v * inv for v in w])
        acc = None
        for r in range(4):
            t = parts[r][0].astype(F32) * wt[:, r:r + 1]
            acc = t if acc is None else acc + t
        o_out[:, hh] = acc.astype(BF).reshape(toks, grp, dim)
        lfin[pl.ds(hh, 1), :] = (m + jnp.log2(tot)) * float(math.log(2.0))

    def final_wait(k):
        for own in (True, False):
            hh = (h if own else oh) * heads + k
            for rel in (LEFT, RIGHT) if own else (0, LEFT, RIGHT, 3):
                arrived(ob.at[rel, hh], ors.at[rel, hh])
                arrived(lb.at[rel, hh], lrs.at[rel, hh])

    def final_both(k):
        final(k, True)
        final(k, False)

    rest = oth_b + new_b
    units = [(k, 0, own_b, own_slot(k, 0)) for k in range(heads)]
    units += [(k, c, all_b, slot_of(k, c)) for k, c in ORDER]
    units += [(k, 0, rest, own_slot(k, 1)) for k in range(heads)]
    nown, total = heads, len(units)
    before = {2: [functools.partial(forwards, 0)], nown - 1: [other_keys, functools.partial(forwards, 1)]}
    for k in range(2, heads):
        before.setdefault(nown + 3 * k - 5, []).append(functools.partial(forwards, k))
    merge_at = {11: 0, 13: 1, 15: 2, 17: 3}

    def send(i):
        k, c, b, u = units[i]
        if c == 0:
            start(own_copies(k, 0 if i < nown else 1))
        elif c == FAR:
            start(far_copies(k, 0))
            start(far_copies(k, 1))
        else:
            start(side_copies(k, c))

    wait_q(0, 0)
    step(1, None, (0, 0, own_b))
    for i in range(total):
        for f in before.get(i, ()):
            f()
        k, c, b, u = units[i]
        nxt = None
        if i + 1 < total:
            k2, c2_, b2, _ = units[i + 1]
            if not (c2_ == 0 and i + 1 >= nown):
                wait_q(k2, c2_)
            nxt = (k2, c2_, b2)
        extras = []
        if i > 0:
            extras.append(functools.partial(close, units[i - 1][3], (i - 1) % 2))
        r = merge_at.get(i)
        if r is not None:
            relay_wait(r)
            extras.append(functools.partial(relay_merge, r))
        if i == total - 1:
            final_wait(0)
            extras.append(functools.partial(final_both, 0))
        step(i % 2, (k, b), nxt, extras)
        if i > 0:
            send(i - 1)
        if r is not None:
            relay_send(r)
    final_wait(1)
    close(units[-1][3], (total - 1) % 2)
    final_both(1)
    send(total - 1)
    for k in range(2, heads):
        final_wait(k)
    for k in range(2, heads):
        final_both(k)

    kh = 2 * heads
    ltr[...] = jnp.concatenate([lfin[...], jnp.zeros((128 - kh, rows), F32)], axis=0).T
    lse = None
    for g in range(grp):
        one = (lax.broadcasted_iota(jnp.int32, (128, kh * grp), 0) * grp + g == lax.broadcasted_iota(jnp.int32, (128, kh * grp), 1))
        t = jnp.dot(ltr[pl.ds(g, toks, stride=grp), :], one.astype(F32), preferred_element_type=F32, precision=lax.Precision.HIGHEST)
        lse = t if lse is None else lse + t
    l_out[...] = lse

    for buf, sem in ((qb.at[0:7 * heads // 2], qss), (osend.at[0:3 * heads], oss), (lsend.at[0:3 * heads], lss),
                     (orel.at[0], rss), (lrel.at[0], rls), (kst.at[0:cl], kvs.at[0]), (vst.at[0:cl], kvs.at[1])):
        arrived(buf, sem)
    for cp in new_remote():
        cp.wait_send()


def solution(mesh):
    n = mesh.shape['cp']
    tok = P(('dp', 'cp'))

    def local(queries, key_new, value_new, key_cache, value_cache, prefix_len):
        t, qh, d = queries.shape
        cl, kh = key_cache.shape[0], key_cache.shape[1]
        g = qh // kh
        hv = kh // 2
        rows = t * g
        nkeys = 2 * cl + 2 * t
        width = -(-nkeys // 128) * 128
        q = queries.reshape(t, 2, hv, g, d)
        kc, vc = (a.reshape(cl, 2, hv, d) for a in (key_cache, value_cache))
        kn, vn = (a.reshape(t, 2, hv, d) for a in (key_new, value_new))
        anyspec = pl.BlockSpec(memory_space=pltpu.HBM)
        vm = pl.BlockSpec(memory_space=pltpu.VMEM)
        dma = pltpu.SemaphoreType.DMA
        nres = 5 * hv
        o, l = pl.pallas_call(
            functools.partial(attend_kernel, n, d ** -0.5),
            name='attend',
            out_shape=(jax.ShapeDtypeStruct((t, kh, g, d), BF), jax.ShapeDtypeStruct((t, qh), F32)),
            in_specs=[pl.BlockSpec(memory_space=pltpu.SMEM)] + [anyspec] * 5,
            out_specs=(vm, vm),
            scratch_shapes=[
                pltpu.VMEM((hv, nkeys, d), BF),
                pltpu.VMEM((hv, d, width), BF),
                pltpu.VMEM((2 * cl, hv, d), BF),
                pltpu.VMEM((2 * cl, hv, d), BF),
                pltpu.VMEM((2 * t, hv, d), BF),
                pltpu.VMEM((2 * t, hv, d), BF),
                pltpu.VMEM((2, PREP * hv, d), F32),
                pltpu.VMEM((4 * hv, 2 * t, g, d), BF),
                pltpu.VMEM((4, kh, rows, d), BF),
                pltpu.VMEM((4, kh, 1, rows), F32),
                pltpu.VMEM((nres, 2 * rows, d), BF),
                pltpu.VMEM((nres, 2, 1, rows), F32),
                pltpu.VMEM((2, 2 * hv, rows, d), BF),
                pltpu.VMEM((2, 2 * hv, 1, rows), F32),
                pltpu.VMEM((nkeys, 2 * rows), F32),
                pltpu.VMEM((nkeys, 2 * rows), F32),
                pltpu.VMEM((2, 8, 2 * rows), F32),
                pltpu.VMEM((kh, rows), F32),
                pltpu.VMEM((rows, 128), F32),
                pltpu.VMEM((2 * cl, 128), F32),
                pltpu.VMEM((2, d, 2 * rows), F32),
                pltpu.VMEM((2, 8, 2 * rows), F32),
                dma((2, PARTS)), dma((2,)), dma((2, PARTS)),
                dma((2,)), dma((2,)), dma((2,)),
                dma, dma((4, 2, hv)),
                dma, dma((4, kh)), dma, dma((4, kh)),
                dma, dma((2, hv)), dma, dma((2, hv)),
            ],
            compiler_params=pltpu.CompilerParams(collective_id=0, has_side_effects=True,
                                                 vmem_limit_bytes=40 * 2 ** 20),
        )(prefix_len, *[pltpu.with_memory_space_constraint(a, pltpu.HBM) for a in (q, kn, vn, kc, vc)])
        return o.reshape(t, qh, d), l

    return jax.shard_map(local, mesh=mesh, in_specs=(tok, tok, tok, tok, tok, P('dp')), out_specs=(tok, tok), check_vma=False)
```

```python
import functools
import math

import jax
import jax.numpy as jnp
from jax import lax
from jax.experimental import pallas as pl
from jax.experimental.pallas import tpu as pltpu
from jax.sharding import PartitionSpec as P

MESH = pl.DeviceIdType.MESH
NEG = -1e30
CH = 256
PREP = 256
PARTS = 3
BF = jnp.bfloat16
F32 = jnp.float32
LEFT, RIGHT, FAR = 1, 2, 3
ORDER = ((0, FAR), (0, LEFT), (0, RIGHT), (1, FAR), (1, LEFT), (1, RIGHT),
         (2, FAR), (2, LEFT), (3, FAR), (2, RIGHT), (3, LEFT), (3, RIGHT))
def attend_kernel(n, scale, plen, q, kn, vn, kc, vc, o_out, l_out,
                  kb, vb, kst, vst, knst, vnst, prep, qb, ob, lb, osend, lsend, orel, lrel, s0, s1, mscr, lfin, ltr, lim, oacc, lacc,
                  kvl, kvs, kvr, nvl, nvs, nvr, qss, qrs, oss, ors, lss, lrs, rss, rrs, rls, rlr):
    S = (s0, s1)
    toks, heads, grp, dim = q.shape[0], q.shape[2], q.shape[3], q.shape[4]
    rows = toks * grp
    cols = 2 * rows
    cl = kc.shape[0]
    c2 = float(scale * math.log2(math.e))
    nch = n // 2
    me = lax.axis_index('cp')
    x, h = me // 2, lax.rem(me, 2)
    oh = 1 - h
    xl, xr, xd = lax.rem(x + nch - 1, nch), lax.rem(x + 1, nch), lax.rem(x + 2, nch)
    chips = (x, xl, xr, xd)

    def remote(src, dst, ss, rs, chip, core):
        return pltpu.make_async_remote_copy(src_ref=src, dst_ref=dst, send_sem=ss, recv_sem=rs,
                                            device_id={'cp': chip * 2 + core}, device_id_type=MESH)

    def arrived(dst, sem):
        pltpu.make_async_copy(dst, dst, sem).wait()

    bar = pltpu.get_barrier_semaphore()
    for j in range(1, n):
        pl.semaphore_signal(bar, inc=1, device_id={'cp': lax.rem(me + j, n)}, device_id_type=MESH)

    part = cl // PARTS

    def kv_local(p):
        src = pl.ds(p * part, part)
        return [pltpu.make_async_copy(a.at[src, h], st.at[src], kvl.at[i, p]) for i, (a, st) in enumerate(((kc, kst), (vc, vst)))]

    def kv_remote(p):
        src, dst = pl.ds(p * part, part), pl.ds(cl + p * part, part)
        return [remote(a.at[src, oh], st.at[dst], kvs.at[i], kvr.at[i, p], x, oh) for i, (a, st) in enumerate(((kc, kst), (vc, vst)))]

    def kv_arrived(p):
        dst = pl.ds(cl + p * part, part)
        for i, st in enumerate((kst, vst)):
            arrived(st.at[dst], kvr.at[i, p])

    nrow = pl.ds(h * toks, toks)

    def new_local():
        return [pltpu.make_async_copy(a.at[:, h], st.at[nrow], nvl.at[i]) for i, (a, st) in enumerate(((kn, knst), (vn, vnst)))]

    def new_remote():
        return [remote(a.at[:, oh], st.at[nrow], nvs.at[i], nvr.at[i], x, oh) for i, (a, st) in enumerate(((kn, knst), (vn, vnst)))]

    def q_local(k):
        return pltpu.make_async_copy(q.at[:, h, k], qb.at[k, nrow], qrs.at[0, h, k])

    def q_partner(k):
        return remote(q.at[:, oh, k], qb.at[k, nrow], qss, qrs.at[0, h, k], x, oh)

    def q_remote(k):
        out = []
        for chip, rel in ((xl, RIGHT), (xr, LEFT)):
            for core in (0, 1):
                out.append(remote(q.at[:, core, k], qb.at[rel * heads + k, nrow], qss, qrs.at[rel, h, k], chip, core))
        return out

    def q_arrived(rel, core, k):
        arrived(qb.at[rel * heads + k, pl.ds(core * toks, toks)], qrs.at[rel, core, k])

    def forward(k, way):
        rel, chip = ((LEFT, xr), (RIGHT, xl))[way]
        piece = pl.ds(way * toks, toks)
        return remote(qb.at[rel * heads + k, piece], qb.at[FAR * heads + k, piece], qss, qrs.at[FAR, way, k], chip, h)

    def forwards(k):
        for way, rel in ((0, LEFT), (1, RIGHT)):
            q_arrived(rel, way, k)
            forward(k, way).start()
        if k + heads // 2 < heads:
            for cp in q_remote(k + heads // 2):
                cp.start()

    for p in range(PARTS):
        for cp in kv_local(p):
            cp.start()
    for cp in new_local():
        cp.start()
    for k in range(heads):
        q_local(k).start()
    pl.semaphore_wait(bar, n - 1)
    for k in range(heads):
        q_partner(k).start()
    for cp in new_remote():
        cp.start()
    for k in range(heads // 2):
        for cp in q_remote(k):
            cp.start()
    for p in range(PARTS):
        for cp in kv_remote(p):
            cp.start()

    pref = plen[0] - x * (2 * cl)

    def split(kraw, vraw, count, base, valid=None):
        prep[0, 0:count * heads] = kraw.reshape(count * heads, dim).astype(F32)
        prep[1, 0:count * heads] = vraw.reshape(count * heads, dim).astype(F32)

        def rows_of(w, j):
            v = prep[w, pl.ds(j, count, stride=heads), :]
            if valid is not None:
                v = jnp.where(lax.broadcasted_iota(jnp.int32, (count, 1), 0) < valid, v, 0.0)
            return v.astype(BF)

        for j in range(heads):
            kb[j, pl.ds(base, count), :] = rows_of(0, j)
            vb[j, :, pl.ds(base, count)] = rows_of(1, j).T

    def split_part(first, start_pos):
        for may_hide in (False, True):
            @pl.when(4 * (x + 1) > 3 * nch if may_hide else 4 * (x + 1) <= 3 * nch)
            def _(may_hide=may_hide):
                def go(i, carry):
                    base = pl.multiple_of(first + i * PREP, PREP)
                    valid = pref - (start_pos + i * PREP)
                    split(kst[pl.ds(base, PREP)], vst[pl.ds(base, PREP)], PREP, base, valid if may_hide else None)
                    lim[pl.ds(base, PREP), :] = jnp.where(lax.broadcasted_iota(jnp.int32, (PREP, 128), 0) < valid, float(jnp.finfo(F32).max), NEG)
                    return carry
                lax.fori_loop(0, part // PREP, go, 0)

    own_b = [(a, a + CH) for a in range(0, cl, CH)]
    oth_b = [(a, a + CH) for a in range(cl, 2 * cl, CH)]
    new_b = [(2 * cl, 2 * cl + 2 * toks)]
    all_b = own_b + oth_b + new_b

    def score_chunk(k, qv, chip, a, e, dst, mx):
        s = lax.dot_general(kb[k, a:e, :], qv, (((1,), (1,)), ((), ())), preferred_element_type=F32)
        if a < 2 * cl:
            s = jnp.minimum(s, jnp.concatenate([lim[a:e, :]] * (cols // 128), axis=1))
        else:
            key = lax.broadcasted_iota(jnp.int32, (e - a, cols), 0)
            tok = lax.broadcasted_iota(jnp.int32, (e - a, cols), 1) // grp
            s = jnp.where(key - tok <= (chip - x) * (2 * toks), s, NEG)
        dst[a:e, :] = s
        mb = jnp.max(s.reshape((e - a) // 8, 8, cols), axis=0)
        return mb if mx is None else jnp.maximum(mx, mb)

    def value_chunk(k, a, e, src, mc, o, l):
        p = jnp.exp2(src[a:e, :] * c2 - mc)
        lsum = jnp.sum(p.reshape((e - a) // 8, 8, cols), axis=0)
        pp = p.astype(BF)
        if cols % 256:
            pp = jnp.concatenate([pp, pp[:, :256 - cols % 256]], axis=1)
        oo = jnp.dot(vb[k, :, a:e], pp, preferred_element_type=F32)
        return (oo if o is None else o + oo), (lsum if l is None else l + lsum)

    def step(slot, cur, nxt, extras=()):
        mx = o = l = None
        if nxt is not None:
            k2, r2, b2 = nxt
            qv = qb[r2 * heads + k2].reshape(cols, dim)
        if cur is not None:
            k, b1 = cur
            mc = mscr[slot][0:1, :]
        count = max(len(b2) if nxt is not None else 0, len(b1) if cur is not None else 0)
        for i in range(count):
            if nxt is not None and i < len(b2):
                mx = score_chunk(k2, qv, chips[r2], *b2[i], S[1 - slot], mx)
            if cur is not None and i < len(b1):
                o, l = value_chunk(k, *b1[i], S[slot], mc, o, l)
            for j, extra in enumerate(extras):
                if i == min(1 + 2 * j, count - 1):
                    extra()
        if nxt is not None:
            mscr[1 - slot] = jnp.broadcast_to(jnp.max(mx, axis=0, keepdims=True) * c2, (8, cols))
        if cur is not None:
            ls = jnp.sum(l, axis=0, keepdims=True)
            oacc[slot] = o[:, :cols]
            lacc[slot, 0:1] = 1.0 / ls
            lacc[slot, 1:2] = mc + jnp.log2(ls)

    def close(u, slot):
        osend[u] = (oacc[slot] * lacc[slot, 0:1]).T.astype(BF)
        lse = lacc[slot, 1:2]
        lsend[u, 0] = lse[:, :rows]
        lsend[u, 1] = lse[:, rows:]

    def slot_of(k, c):
        return k * 3 + (c - 1)

    def own_slot(k, half):
        return heads * 3 + half * heads + k

    def piece(a):
        return pl.ds(pl.multiple_of(a * rows, 16), rows)

    def result(u, a, dst_o, dst_l, so, sl, chip, core):
        return (remote(osend.at[u, piece(a)], dst_o, oss, so, chip, core),
                remote(lsend.at[u, a], dst_l, lss, sl, chip, core))

    hh_of = lambda k: h * heads + k

    def own_copies(k, half):
        hh = hh_of(k)
        rel = 3 * half
        return result(own_slot(k, half), oh, ob.at[rel, hh], lb.at[rel, hh], ors.at[rel, hh], lrs.at[rel, hh], x, oh)

    def side_copies(k, c):
        hh = hh_of(k)
        a, rel, chip = (c - 1), 3 - c, chips[c]
        return result(slot_of(k, c), a, ob.at[rel, hh], lb.at[rel, hh], ors.at[rel, hh], lrs.at[rel, hh], chip, a)

    def far_copies(k, a):
        chip = (xr, xl)[a]
        return result(slot_of(k, FAR), a, orel.at[a, k], lrel.at[a, k], rrs.at[a, k], rlr.at[a, k], chip, h)

    def merged_copies(k, a):
        hh = hh_of(k)
        chip, rel = ((xr, LEFT), (xl, RIGHT))[a]
        return (remote(orel.at[a, heads + k], ob.at[rel, hh], rss, ors.at[rel, hh], chip, a),
                remote(lrel.at[a, heads + k], lb.at[rel, hh], rls, lrs.at[rel, hh], chip, a))

    def columns(ws):
        pad = jnp.zeros((8 - len(ws), rows), F32)
        return jnp.concatenate(list(ws) + [pad], axis=0).T

    def relay_wait(k):
        for a in (0, 1):
            arrived(orel.at[a, k], rrs.at[a, k])
            arrived(lrel.at[a, k], rlr.at[a, k])

    def relay_merge(k):
        for a in (0, 1):
            u = slot_of(k, (RIGHT, LEFT)[a])
            l0, l1 = lsend[u, a], lrel[a, k]
            m = jnp.maximum(l0, l1)
            w0, w1 = jnp.exp2(l0 - m), jnp.exp2(l1 - m)
            tot = w0 + w1
            inv = 1.0 / tot
            wt = columns((w0 * inv, w1 * inv))
            orel[a, heads + k] = (osend[u, a * rows:(a + 1) * rows, :].astype(F32) * wt[:, 0:1]
                                  + orel[a, k].astype(F32) * wt[:, 1:2]).astype(BF)
            lrel[a, heads + k] = m + jnp.log2(tot)

    def relay_send(k):
        for a in (0, 1):
            for cp in merged_copies(k, a):
                cp.start()

    def start(cps):
        for cp in cps:
            cp.start()

    def wait_q(k, c):
        if c != LEFT:
            q_arrived(c, 0, k)
        if c != RIGHT:
            q_arrived(c, 1, k)

    for p in range(PARTS):
        for cp in kv_local(p):
            cp.wait()
        split_part(p * part, h * cl + p * part)

    def other_keys():
        for cp in new_local():
            cp.wait()
        for i, st in enumerate((knst, vnst)):
            arrived(st.at[pl.ds(oh * toks, toks)], nvr.at[i])
        split(knst[...], vnst[...], 2 * toks, 2 * cl)
        for p in range(PARTS):
            kv_arrived(p)
            split_part(cl + p * part, oh * cl + p * part)

    def final(k, own):
        hh = (h if own else oh) * heads + k
        if own:
            parts = [(osend[own_slot(k, half), piece(h), :], lsend[own_slot(k, half), h]) for half in (0, 1)]
        else:
            parts = [(ob[rel, hh], lb[rel, hh]) for rel in (0, 3)]
        parts += [(ob[rel, hh], lb[rel, hh]) for rel in (LEFT, RIGHT)]
        ls = [p[1] for p in parts]
        m = jnp.maximum(jnp.maximum(ls[0], ls[1]), jnp.maximum(ls[2], ls[3]))
        w = [jnp.exp2(v - m) for v in ls]
        tot = (w[0] + w[1]) + (w[2] + w[3])
        inv = 1.0 / tot
        wt = columns([v * inv for v in w])
        acc = None
        for r in range(4):
            t = parts[r][0].astype(F32) * wt[:, r:r + 1]
            acc = t if acc is None else acc + t
        o_out[:, hh] = acc.astype(BF).reshape(toks, grp, dim)
        lfin[pl.ds(hh, 1), :] = (m + jnp.log2(tot)) * float(math.log(2.0))

    def final_wait(k):
        for own in (True, False):
            hh = (h if own else oh) * heads + k
            for rel in (LEFT, RIGHT) if own else (0, LEFT, RIGHT, 3):
                arrived(ob.at[rel, hh], ors.at[rel, hh])
                arrived(lb.at[rel, hh], lrs.at[rel, hh])

    def final_both(k):
        final(k, True)
        final(k, False)

    rest = oth_b + new_b
    units = [(k, 0, own_b, own_slot(k, 0)) for k in range(heads)]
    units += [(k, c, all_b, slot_of(k, c)) for k, c in ORDER]
    units += [(k, 0, rest, own_slot(k, 1)) for k in range(heads)]
    nown, total = heads, len(units)
    before = {1: [functools.partial(forwards, 0)], nown - 1: [other_keys, functools.partial(forwards, 1)]}
    for k in range(2, heads):
        before.setdefault(nown + 3 * (k - 2) + 1, []).append(functools.partial(forwards, k))
    merge_at = {nown + 3 * k + 5: k for k in range(heads - 1)}
    merge_at[total - heads + 1] = heads - 1

    def send(i):
        k, c, b, u = units[i]
        if c == 0:
            start(own_copies(k, 0 if i < nown else 1))
        elif c == FAR:
            start(far_copies(k, 0))
            start(far_copies(k, 1))
        else:
            start(side_copies(k, c))

    wait_q(0, 0)
    step(1, None, (0, 0, own_b))
    for i in range(total):
        for f in before.get(i, ()):
            f()
        k, c, b, u = units[i]
        nxt = None
        if i + 1 < total:
            k2, c2_, b2, _ = units[i + 1]
            if not (c2_ == 0 and i + 1 >= nown):
                wait_q(k2, c2_)
            nxt = (k2, c2_, b2)
        extras = []
        if i > 0:
            extras.append(functools.partial(close, units[i - 1][3], (i - 1) % 2))
        r = merge_at.get(i)
        if r is not None:
            relay_wait(r)
            extras.append(functools.partial(relay_merge, r))
        if i == total - 1:
            final_wait(0)
            extras.append(functools.partial(final_both, 0))
        step(i % 2, (k, b), nxt, extras)
        if i > 0:
            send(i - 1)
        if r is not None:
            relay_send(r)
    final_wait(1)
    close(units[-1][3], (total - 1) % 2)
    final_both(1)
    send(total - 1)
    for k in range(2, heads):
        final_wait(k)
        final_both(k)

    kh = 2 * heads
    ltr[...] = jnp.concatenate([lfin[...], jnp.zeros((128 - kh, rows), F32)], axis=0).T
    lse = None
    for g in range(grp):
        one = (lax.broadcasted_iota(jnp.int32, (128, kh * grp), 0) * grp + g == lax.broadcasted_iota(jnp.int32, (128, kh * grp), 1))
        t = jnp.dot(ltr[pl.ds(g, toks, stride=grp), :], one.astype(F32), preferred_element_type=F32, precision=lax.Precision.HIGHEST)
        lse = t if lse is None else lse + t
    l_out[...] = lse

    for buf, sem in ((qb.at[0:7 * heads // 2], qss), (osend.at[0:3 * heads], oss), (lsend.at[0:3 * heads], lss),
                     (orel.at[0], rss), (lrel.at[0], rls), (kst.at[0:cl], kvs.at[0]), (vst.at[0:cl], kvs.at[1])):
        arrived(buf, sem)
    for cp in new_remote():
        cp.wait_send()


def solution(mesh):
    n = mesh.shape['cp']
    tok = P(('dp', 'cp'))

    def local(queries, key_new, value_new, key_cache, value_cache, prefix_len):
        t, qh, d = queries.shape
        cl, kh = key_cache.shape[0], key_cache.shape[1]
        g = qh // kh
        hv = kh // 2
        rows = t * g
        nkeys = 2 * cl + 2 * t
        width = -(-nkeys // 128) * 128
        q = queries.reshape(t, 2, hv, g, d)
        kc, vc = (a.reshape(cl, 2, hv, d) for a in (key_cache, value_cache))
        kn, vn = (a.reshape(t, 2, hv, d) for a in (key_new, value_new))
        anyspec = pl.BlockSpec(memory_space=pltpu.HBM)
        vm = pl.BlockSpec(memory_space=pltpu.VMEM)
        dma = pltpu.SemaphoreType.DMA
        nres = 5 * hv
        o, l = pl.pallas_call(
            functools.partial(attend_kernel, n, d ** -0.5),
            name='attend',
            out_shape=(jax.ShapeDtypeStruct((t, kh, g, d), BF), jax.ShapeDtypeStruct((t, qh), F32)),
            in_specs=[pl.BlockSpec(memory_space=pltpu.SMEM)] + [anyspec] * 5,
            out_specs=(vm, vm),
            scratch_shapes=[
                pltpu.VMEM((hv, nkeys, d), BF),
                pltpu.VMEM((hv, d, width), BF),
                pltpu.VMEM((2 * cl, hv, d), BF),
                pltpu.VMEM((2 * cl, hv, d), BF),
                pltpu.VMEM((2 * t, hv, d), BF),
                pltpu.VMEM((2 * t, hv, d), BF),
                pltpu.VMEM((2, PREP * hv, d), F32),
                pltpu.VMEM((4 * hv, 2 * t, g, d), BF),
                pltpu.VMEM((4, kh, rows, d), BF),
                pltpu.VMEM((4, kh, 1, rows), F32),
                pltpu.VMEM((nres, 2 * rows, d), BF),
                pltpu.VMEM((nres, 2, 1, rows), F32),
                pltpu.VMEM((2, 2 * hv, rows, d), BF),
                pltpu.VMEM((2, 2 * hv, 1, rows), F32),
                pltpu.VMEM((nkeys, 2 * rows), F32),
                pltpu.VMEM((nkeys, 2 * rows), F32),
                pltpu.VMEM((2, 8, 2 * rows), F32),
                pltpu.VMEM((kh, rows), F32),
                pltpu.VMEM((rows, 128), F32),
                pltpu.VMEM((2 * cl, 128), F32),
                pltpu.VMEM((2, d, 2 * rows), F32),
                pltpu.VMEM((2, 8, 2 * rows), F32),
                dma((2, PARTS)), dma((2,)), dma((2, PARTS)),
                dma((2,)), dma((2,)), dma((2,)),
                dma, dma((4, 2, hv)),
                dma, dma((4, kh)), dma, dma((4, kh)),
                dma, dma((2, hv)), dma, dma((2, hv)),
            ],
            compiler_params=pltpu.CompilerParams(collective_id=0, has_side_effects=True,
                                                 vmem_limit_bytes=40 * 2 ** 20),
        )(prefix_len, *[pltpu.with_memory_space_constraint(a, pltpu.HBM) for a in (q, kn, vn, kc, vc)])
        return o.reshape(t, qh, d), l

    return jax.shard_map(local, mesh=mesh, in_specs=(tok, tok, tok, tok, tok, P('dp')), out_specs=(tok, tok), check_vma=False)
```
